128 devices in a mesh: section: 4 (over z), dp: 8 (over y, core), mp: 4 (over x).
Axes of the slice: x: 4, y: 4, z: 4, core: 2. Of those that a mesh axis runs over, the one named last changes fastest.
Arguments:
- text: bfloat16 [4, 4096, 4096], P('section', ('dp', 'mp')), may hold values from -6 to 6
- patches: bfloat16 [16384, 1024], P(('section', 'dp')), may hold values from -6 to 6
- segments: int32 [4, 8, 512], P('section', 'dp'), may hold values from 0 to 3, never falling along the last dimension, each value on 1 to 256 neighbouring positions
- loss_mask: int32 [4, 4096], P('section', ('dp', 'mp')), may hold values from 0 to 1, as said below
- tile_batch: int32 [8, 8], P('dp'), may hold values from 0 to 3, as said below
- tile_offset: int32 [8, 8], P('dp'), may hold values from 0 to 448, as said below
- attn_gain: float32 [4, 4096], P('section'), may hold values from 0.5 to 2
- w_query: bfloat16 [4, 4096, 2048], P('section', None, 'mp'), may hold values from -0.09375 to 0.09375
- w_kv: bfloat16 [4, 2, 4096, 512], P('section', None, None, 'mp'), may hold values from -0.09375 to 0.09375
- w_out: bfloat16 [4, 2048, 4096], P('section', 'mp'), may hold values from -0.125 to 0.125
- vis_gain: float32 [2, 1024], replicated, may hold values from 0.5 to 2
- vis_bias: float32 [2, 1024], replicated, may hold values from -3 to 3
- v_qkv: bfloat16 [3, 1024, 1024], P(None, ('section', 'dp'), 'mp'), may hold values from -0.1875 to 0.1875
- v_out: bfloat16 [1024, 1024], P('mp', ('section', 'dp')), may hold values from -0.1875 to 0.1875
- v_up: bfloat16 [1024, 4096], P(('section', 'dp'), 'mp'), may hold values from -0.1875 to 0.1875
- v_down: bfloat16 [4096, 1024], P('mp', ('section', 'dp')), may hold values from -0.09375 to 0.09375
- v_proj: bfloat16 [4096, 4096], P(('section', 'dp'), 'mp'), may hold values from -0.09375 to 0.09375
Outputs:
- hidden: bfloat16 [4, 4096, 4096], P('section', ('dp', 'mp'))
- token_weight: float32 [4, 4096], P('section', ('dp', 'mp'))
The draws below stay inside these ranges and needn't reach their ends.
Inputs may be any that keep to these rules, and one draw needn't show every extreme that they name: `tile_batch`: in every data-parallel index, the 2 tiles of each section index go 1 to each of two different micro-batches; one micro-batch receives 1 tiles from every section index. `tile_offset`: offsets are multiples of 64; the runs of one sequence never intersect. `loss_mask`: the first position of every sequence is a one.
All inputs are finite; a program needn't handle non-finite values.
Results may differ from the reference program's by a relative error of at most 0.025.
Values may be sent and summed in bfloat16 or wider, within the bound.
No kernel may reach another device: no remote copies, remote signals or barrier semaphores. Data moves between devices by JAX's collectives and lax.ppermute only.
A program may use at most 192 MiB of HBM per device.

```python
import math
import jax
import jax.numpy as jnp
import numpy as np
from jax import lax

D = 4096
QH = 16
KVH = 4
HD = 128
VD = 1024
VH = 16
VHD = 64
VFF = 4096
GRID = 16
PATCH = 256
POOL = 64
L = 512
TILES_G = 2
CAP = 1
MICRO = 4
TILES = 64
N_SECTION = 4
N_DP = 8
N_MP = 4


def tile_plan(key):
    base_key = jax.random.fold_in(key, 7)
    target_key, second_key, order_key, slot_key = jax.random.split(base_key, 4)
    tile_count = N_SECTION * TILES_G
    target = jax.random.randint(target_key, (N_DP, 1), 0, MICRO)
    moved = jax.random.randint(second_key, (N_DP, N_SECTION), 1, MICRO)
    second = jnp.mod(target + moved, MICRO)
    orders = jax.vmap(lambda item_key: jax.random.permutation(item_key, TILES_G))(jax.random.split(order_key, N_DP * N_SECTION))
    orders = orders.reshape(N_DP, N_SECTION, TILES_G)
    batches = jnp.where(orders < CAP, target[:, :, None], second[:, :, None]).reshape(N_DP, tile_count)
    tile_ids = jnp.arange(tile_count, dtype=jnp.int32)
    earlier = tile_ids[None, :] < tile_ids[:, None]
    same = batches[:, :, None] == batches[:, None, :]
    ranks = jnp.sum((same & earlier[None, :, :]).astype(jnp.int32), axis=2)
    slot_total = L // POOL
    slot_perm = jax.vmap(lambda item_key: jax.random.permutation(item_key, slot_total))(jax.random.split(slot_key, N_DP * MICRO))
    slot_perm = slot_perm.reshape(N_DP, MICRO * slot_total)
    offsets = POOL * jnp.take_along_axis(slot_perm, batches * slot_total + ranks, axis=1)
    return (batches.astype(jnp.int32), offsets.astype(jnp.int32))


def draw_tile_batch(key, part):
    batches, offsets = tile_plan(key)
    return batches


def draw_tile_offset(key, part):
    batches, offsets = tile_plan(key)
    return offsets


def draw_loss_mask(key, part):
    seq_count = MICRO * N_DP
    seq_index = jnp.arange(seq_count, dtype=jnp.int32)
    threshold = 250 + 500 * seq_index // max(seq_count - 1, 1)
    rolls = jax.random.randint(jax.random.fold_in(key, 5), (seq_count, L), 0, 1000)
    marked = (rolls < threshold[:, None]).astype(jnp.int32)
    leading = (jnp.arange(L) == 0).astype(jnp.int32)
    marked = jnp.maximum(marked, leading[None, :])
    return marked.reshape(MICRO, N_DP * L)


def gain_values(key, shape):
    return jax.random.uniform(key, shape, jnp.float32, 0.5, 1.5)


def draw_attn_gain(key, part):
    return gain_values(jax.random.fold_in(key, 3), (N_SECTION, D))


def draw_vis_gain(key, part):
    return gain_values(jax.random.fold_in(key, 4), (2, VD))


def shard_levels(stream_key, extent, pieces, low, high):
    level, own = 1.0, jax.random.fold_in(stream_key, 6)
    for axis_at, shards_of in pieces:
        heights = jnp.exp(jax.random.uniform(jax.random.fold_in(own, axis_at), (shards_of,), jnp.float32, low / len(pieces), high / len(pieces)))
        level = level * jnp.repeat(heights, extent[axis_at] // shards_of).reshape([-1 if axis == axis_at else 1 for axis in range(len(extent))])
    return level


def split_up(number_of, total, bound, slope):
    loads = [(1 << 20) // math.isqrt(grade ** slope) + 1 for grade in range(2, number_of + 1)]
    surplus, given = total - bound - (number_of - 1), [1] * (number_of - 1)
    while surplus > 0:
        free = [i for i in range(number_of - 1) if given[i] < bound]
        pool, remaining = sum([loads[i] for i in free]), surplus
        for i in free:
            extra = min(bound - given[i], max(1, remaining * loads[i] // pool), surplus)
            given[i] = given[i] + extra
            surplus = surplus - extra
    return np.array([bound] + given)


def uneven(rng, count, total, reach, slope):
    if count == 2:
        one = jax.random.randint(rng, (), max(1, total - reach), min(reach, total - 1) + 1)
        return jnp.stack([one, total - one])
    sizes = jnp.asarray(split_up(count, total, reach, slope), jnp.int32)
    twos = (count - 1) // 2
    source_of, sink = sizes[1:1 + 2 * twos:2], sizes[2:2 + 2 * twos:2]
    margin = jnp.minimum(source_of - 1, reach - sink)
    shifted = jax.random.randint(jax.random.fold_in(rng, 1), (twos,), 0, 1 << 20) % (margin + 1)
    sizes = sizes.at[1:1 + 2 * twos:2].set(source_of - shifted).at[2:2 + 2 * twos:2].set(sink + shifted)
    return sizes[jax.random.permutation(jax.random.fold_in(rng, 2), count)]


def normal_values(stream_key, shape, scale, bound, pieces=(), kind=jnp.bfloat16):
    values = jax.random.normal(stream_key, shape, jnp.float32) * scale
    if len(pieces) > 0:
        values = shard_levels(stream_key, shape, pieces, -0.22, 0.18) * values
    return jnp.clip(values, min=-bound, max=bound).astype(kind)


def setup_inputs(seed: int = 0) -> dict:
    key_list = jax.random.split(jax.random.key(seed), 18)
    return {
        "text": normal_values(key_list[0], (MICRO, N_DP * L, D), 1.0, 6.0, ((0, 4), (1, 32))),
        "patches": normal_values(key_list[1], (TILES * PATCH, VD), 1.0, 6.0, ((0, 32),)),
        "segments": jax.vmap(lambda own: jnp.searchsorted(jnp.cumsum(uneven(own, 4, L, L // 2, 2)), jnp.arange(L), side="right"))(jax.random.split(key_list[2], MICRO * N_DP)).reshape((MICRO, N_DP, L)).astype(jnp.int32),
        "loss_mask": draw_loss_mask(jax.random.fold_in(key_list[17], 71), 0),
        "tile_batch": draw_tile_batch(jax.random.fold_in(key_list[17], 71), 0),
        "tile_offset": draw_tile_offset(jax.random.fold_in(key_list[17], 71), 0),
        "attn_gain": draw_attn_gain(jax.random.fold_in(key_list[17], 71), 0),
        "w_query": normal_values(key_list[7], (N_SECTION, D, QH * HD), D ** -0.5, 0.09375, ((0, 4), (2, 4))),
        "w_kv": normal_values(key_list[8], (N_SECTION, 2, D, KVH * HD), D ** -0.5, 0.09375, ((0, 4), (3, 4))),
        "w_out": normal_values(key_list[9], (N_SECTION, QH * HD, D), (QH * HD) ** -0.5, 0.125, ((0, 4), (1, 4))),
        "vis_gain": draw_vis_gain(jax.random.fold_in(key_list[17], 71), 0),
        "vis_bias": normal_values(key_list[11], (2, VD), 0.5, 3.0, (), jnp.float32),
        "v_qkv": normal_values(key_list[12], (3, VD, VD), VD ** -0.5, 0.1875, ((1, 32), (2, 4))),
        "v_out": normal_values(key_list[13], (VD, VD), VD ** -0.5, 0.1875, ((0, 4), (1, 32))),
        "v_up": normal_values(key_list[14], (VD, VFF), VD ** -0.5, 0.1875, ((0, 32), (1, 4))),
        "v_down": normal_values(key_list[15], (VFF, VD), VFF ** -0.5, 0.09375, ((0, 4), (1, 32))),
        "v_proj": normal_values(key_list[16], (4 * VD, D), (4 * VD) ** -0.5, 0.09375, ((0, 32), (1, 4))),
    }


EPS = 1e-05
ROPE_BASE = 500000.0
BLOCKED = -1e+30

def layer_norm(values, gain, bias):
    wide = values.astype(jnp.float32)
    center = wide - lax.optimization_barrier(jnp.mean(wide, axis=-1, keepdims=True))
    spread = lax.optimization_barrier(jnp.mean(center * center, axis=-1, keepdims=True))
    return (center * lax.rsqrt(spread + EPS) * gain + bias).astype(jnp.bfloat16)

def rms_norm(values, gain):
    wide = values.astype(jnp.float32)
    power = lax.optimization_barrier(jnp.mean(wide * wide, axis=-1, keepdims=True))
    return (wide * lax.rsqrt(power + EPS) * gain).astype(jnp.bfloat16)

def rotate(values, positions):
    half_width = values.shape[-1] // 2
    freqs = ROPE_BASE ** (-2.0 * jnp.arange(half_width, dtype=jnp.float32) / values.shape[-1])
    angles = positions.astype(jnp.float32)[:, None] * freqs[None, :]
    cosine = jnp.cos(angles)[:, None, :]
    sinus_part = jnp.sin(angles)[:, None, :]
    first_half = values[..., :half_width]
    second_half = values[..., half_width:]
    return jnp.concatenate([first_half * cosine - second_half * sinus_part, second_half * cosine + first_half * sinus_part], axis=-1)

def split_sum(left, right):
    row_count = left.shape[0]
    block_width = left.shape[1] // N_MP
    left_blocks = left.reshape(row_count, N_MP, block_width).astype(jnp.float32)
    right_blocks = right.reshape(N_MP, block_width, right.shape[1]).astype(jnp.float32)
    partials = jnp.einsum('rgk,gkn->grn', left_blocks, right_blocks)
    rounded = lax.optimization_barrier(partials.astype(jnp.bfloat16))
    return lax.optimization_barrier(jnp.sum(rounded.astype(jnp.float32), axis=0))

def pixel_shuffle(states):
    tile_count = states.shape[0] // PATCH
    side_half = GRID // 2
    width = states.shape[1]
    arranged = states.reshape(tile_count, side_half, 2, side_half, 2, width)
    return arranged.transpose(0, 1, 3, 2, 4, 5).reshape(tile_count * side_half * side_half, 4 * width)

def encode_group(block, vis_gain, vis_bias, v_qkv, v_out, v_up, v_down, v_proj):
    tile_count = block.shape[0] // PATCH
    normed = layer_norm(block, vis_gain[0], vis_bias[0])
    projected = [jnp.dot(normed, v_qkv[index], preferred_element_type=jnp.float32).astype(jnp.bfloat16).reshape(tile_count, PATCH, VH, VHD) for index in range(3)]
    scores = jnp.einsum('tqhd,tkhd->thqk', projected[0].astype(jnp.float32), projected[1].astype(jnp.float32)) * VHD ** (-0.5)
    probs = jax.nn.softmax(scores, axis=-1).astype(jnp.bfloat16)
    mixed = jnp.einsum('thqk,tkhd->tqhd', probs.astype(jnp.float32), projected[2].astype(jnp.float32)).astype(jnp.bfloat16).reshape(tile_count * PATCH, VD)
    residual = (block.astype(jnp.float32) + split_sum(mixed, v_out)).astype(jnp.bfloat16)
    normed_two = layer_norm(residual, vis_gain[1], vis_bias[1])
    inner = jax.nn.gelu(jnp.dot(normed_two, v_up, preferred_element_type=jnp.float32), approximate=False).astype(jnp.bfloat16)
    states = (residual.astype(jnp.float32) + split_sum(inner, v_down)).astype(jnp.bfloat16)
    return jnp.dot(pixel_shuffle(states), v_proj, preferred_element_type=jnp.float32).astype(jnp.bfloat16)

def decoder_layer(state, segment_ids, gain, w_query, w_kv, w_out):
    length = state.shape[0]
    positions = jnp.arange(length, dtype=jnp.int32)
    normed = rms_norm(state, gain)
    query = rotate(jnp.dot(normed, w_query, preferred_element_type=jnp.float32).reshape(length, QH, HD), positions).astype(jnp.bfloat16)
    keyed = rotate(jnp.dot(normed, w_kv[0], preferred_element_type=jnp.float32).reshape(length, KVH, HD), positions).astype(jnp.bfloat16)
    valued = jnp.dot(normed, w_kv[1], preferred_element_type=jnp.float32).astype(jnp.bfloat16).reshape(length, KVH, HD)
    grouped = query.reshape(length, KVH, QH // KVH, HD).astype(jnp.float32)
    scores = jnp.einsum('qkgd,skd->kgqs', grouped, keyed.astype(jnp.float32)) * HD ** (-0.5)
    allowed = (segment_ids[:, None] == segment_ids[None, :]) & (positions[None, :] <= positions[:, None])
    scores = jnp.where(allowed, scores, BLOCKED)
    probs = jax.nn.softmax(scores, axis=-1).astype(jnp.bfloat16)
    mixed = jnp.einsum('kgqs,skd->qkgd', probs.astype(jnp.float32), valued.astype(jnp.float32)).astype(jnp.bfloat16).reshape(length, QH * HD)
    return (state.astype(jnp.float32) + split_sum(mixed, w_out)).astype(jnp.bfloat16)

def reference(text, patches, segments, loss_mask, tile_batch, tile_offset, attn_gain, w_query, w_kv, w_out, vis_gain, vis_bias, v_qkv, v_out, v_up, v_down, v_proj):
    group_count = N_SECTION * N_DP
    grouped = patches.reshape(group_count, TILES_G * PATCH, VD)
    embedded = lax.map(lambda block: encode_group(block, vis_gain, vis_bias, v_qkv, v_out, v_up, v_down, v_proj), grouped)
    per_tile = embedded.reshape(N_SECTION, N_DP, TILES_G, POOL, D).transpose(1, 0, 2, 3, 4).reshape(N_DP, N_SECTION * TILES_G, POOL, D)
    states = text.reshape(MICRO, N_DP, L, D)
    places = tile_offset[:, :, None] + jnp.arange(POOL, dtype=jnp.int32)[None, None, :]
    dp_ids = jnp.broadcast_to(jnp.arange(N_DP, dtype=jnp.int32)[:, None, None], places.shape)
    micro_ids = jnp.broadcast_to(tile_batch[:, :, None], places.shape)
    states = states.at[micro_ids, dp_ids, places].set(per_tile)
    flat_states = states.reshape(MICRO * N_DP, L, D)
    flat_segments = segments.reshape(MICRO * N_DP, L)

    def run_sequence(pair):
        state, segment_ids = pair
        for layer_index in range(N_SECTION):
            state = decoder_layer(state, segment_ids, attn_gain[layer_index], w_query[layer_index], w_kv[layer_index], w_out[layer_index])
        return state
    hidden = lax.map(run_sequence, (flat_states, flat_segments)).reshape(MICRO, N_DP * L, D)
    weights = loss_mask.astype(jnp.float32)
    token_weight = weights * (MICRO * N_DP * L) / jnp.sum(weights)
    return (hidden, token_weight)
```

```python
import jax
import jax.numpy as jnp
from jax import lax
from jax.sharding import Mesh
from jax.sharding import PartitionSpec as P

HD = 128
VHD = 64
GRID = 16
PATCH = 256
POOL = 64
SECTION_DP = ("section", "dp_0", "dp_1")
MP_FIRST = ("mp", "section", "dp_0", "dp_1")
SECTION_DP_MP = ("section", "dp_0", "dp_1", "mp")
DP = ("dp_0", "dp_1")
DP_MP = ("dp_0", "dp_1", "mp")


EPS = 1e-05
ROPE_BASE = 500000.0
BLOCKED = -1e30


def dot(left, right):
    return jnp.dot(left, right, preferred_element_type=jnp.float32)


def exchange(blocks, axis):
    return lax.all_to_all(blocks, axis, split_axis=0, concat_axis=0, tiled=True)


def everywhere(array, axis):
    return exchange(jnp.broadcast_to(array, (lax.axis_size(axis), *array.shape)), axis)


def over_axes(array, axes):
    for axis in axes:
        array = lax.psum(array, axis)
    return array


def layer_norm(values, gain, bias):
    wide = values.astype(jnp.float32)
    center = wide - jnp.mean(wide, axis=-1, keepdims=True)
    spread = jnp.mean(center * center, axis=-1, keepdims=True)
    return (center * lax.rsqrt(spread + EPS) * gain + bias).astype(jnp.bfloat16)


def rms_norm(values, gain):
    wide = values.astype(jnp.float32)
    power = jnp.mean(wide * wide, axis=-1, keepdims=True)
    return (wide * lax.rsqrt(power + EPS) * gain).astype(jnp.bfloat16)


def rope_tables(length):
    half = HD // 2
    freqs = ROPE_BASE ** (-2.0 * jnp.arange(half, dtype=jnp.float32) / HD)
    angles = jnp.arange(length, dtype=jnp.float32)[:, None] * freqs[None, :]
    return jnp.cos(angles), jnp.sin(angles)


def rotate(values, cosine, sine):
    half = HD // 2
    first, second = values[:, :half], values[:, half:]
    return jnp.concatenate(
        [first * cosine - second * sine, second * cosine + first * sine], axis=1
    ).astype(jnp.bfloat16)


def pixel_shuffle(states):
    rows, width = states.shape
    side_half = GRID // 2
    arranged = states.reshape(rows // (2 * GRID), 2, side_half, 2, width)
    return arranged.transpose(0, 2, 1, 3, 4).reshape(rows // 4, 4 * width)


def summed_rows(partial):
    parts = lax.axis_size("mp")
    blocks = partial.astype(jnp.bfloat16).reshape(parts, -1, partial.shape[1])
    return jnp.sum(exchange(blocks, "mp").astype(jnp.float32), axis=0)


def encode_tiles(patches, vis_gain, vis_bias, slabs, part_at):
    up = slabs[:, 0:32].reshape(1024, 1024)
    down_t = slabs[:, 32:64].reshape(1024, 1024)
    proj = slabs[:, 64:192].reshape(4096, 1024)
    qkv = slabs[:, 192:224, :768].reshape(1024, 768)
    out_t = slabs[:, 192:224, 768:].reshape(1024, 256)
    tile_count = patches.shape[0] // PATCH
    local_width = qkv.shape[1] // 3
    head_count = local_width // VHD
    normed = layer_norm(patches, vis_gain[0], vis_bias[0])
    projected = dot(normed, qkv).astype(jnp.bfloat16)
    query, keyed, valued = (
        projected[:, i * local_width : (i + 1) * local_width].reshape(
            tile_count, PATCH, head_count, VHD
        )
        for i in range(3)
    )
    scores = jnp.einsum(
        "tqhd,tkhd->thqk", query, keyed, preferred_element_type=jnp.float32
    ) * VHD ** (-0.5)
    probs = jax.nn.softmax(scores, axis=-1).astype(jnp.bfloat16)
    mixed = (
        jnp.einsum("thqk,tkhd->tqhd", probs, valued, preferred_element_type=jnp.float32)
        .astype(jnp.bfloat16)
        .reshape(tile_count * PATCH, local_width)
    )
    contract_last = (((1,), (1,)), ((), ()))
    attended = summed_rows(
        lax.dot_general(mixed, out_t, contract_last, preferred_element_type=jnp.float32)
    )
    own_rows = attended.shape[0]
    own = lax.dynamic_slice_in_dim(patches, part_at * own_rows, own_rows, 0)
    residual = (own.astype(jnp.float32) + attended).astype(jnp.bfloat16)
    normed_two = everywhere(layer_norm(residual, vis_gain[1], vis_bias[1]), "mp").reshape(
        patches.shape
    )
    inner = jax.nn.gelu(dot(normed_two, up), approximate=False).astype(jnp.bfloat16)
    fed = summed_rows(
        lax.dot_general(inner, down_t, contract_last, preferred_element_type=jnp.float32)
    )
    states = (residual.astype(jnp.float32) + fed).astype(jnp.bfloat16)
    pooled = everywhere(pixel_shuffle(states), "mp").reshape(-1, 4 * states.shape[1])
    return dot(pooled, proj).astype(jnp.bfloat16)


def attend(state, allowed, cosine, sine, gain, w_joined):
    normed = rms_norm(state, gain)
    joined = dot(normed, w_joined)
    heads = w_joined.shape[1] // HD - 2
    keyed = rotate(joined[:, heads * HD : (heads + 1) * HD], cosine, sine)
    valued = joined[:, (heads + 1) * HD :].astype(jnp.bfloat16)
    mixes = []
    for head in range(heads):
        query = rotate(joined[:, head * HD : (head + 1) * HD], cosine, sine)
        scores = lax.dot_general(
            query, keyed, (((1,), (1,)), ((), ())), preferred_element_type=jnp.float32
        ) * HD ** (-0.5)
        scores = jnp.where(allowed, scores, BLOCKED)
        probs = jax.nn.softmax(scores, axis=-1).astype(jnp.bfloat16)
        mixes.append(dot(probs, valued).astype(jnp.bfloat16))
    return jnp.concatenate(mixes, axis=1)


def shards(
    text,
    patches,
    segments,
    loss_mask,
    tile_batch,
    tile_offset,
    attn_gain,
    w_query,
    w_kv,
    w_out,
    vis_gain,
    vis_bias,
    v_qkv,
    v_out,
    v_up,
    v_down,
    v_proj,
):
    sections = lax.axis_size("section")
    section_at = lax.axis_index("section")
    part_at = lax.axis_index("mp")
    dp_at = lax.axis_index(DP)
    dp_size = lax.axis_size(DP)
    length = segments.shape[2]

    qkv_rows = jnp.concatenate([v_qkv[0], v_qkv[1], v_qkv[2], v_out.T], axis=1)
    slab = jnp.concatenate([v_up, v_down.T, v_proj, qkv_rows], axis=0)
    slabs = lax.all_gather(slab, SECTION_DP)

    totals = over_axes(jnp.sum(loss_mask), SECTION_DP_MP)
    gains = lax.all_gather(attn_gain, "section", axis=0, tiled=True)
    own_out = w_out[0]
    rows_each = own_out.shape[0] // (sections * dp_size)
    out_blocks = own_out.reshape(sections, dp_size, rows_each, -1)
    out_blocks = lax.dynamic_index_in_dim(out_blocks, dp_at, 1, keepdims=False)
    out_blocks = exchange(out_blocks, "section")
    text_full = everywhere(text[0], "mp").reshape(length, -1)
    totals, gains, out_blocks, text_full, slabs, patches = lax.optimization_barrier(
        (totals, gains, out_blocks, text_full, slabs, patches)
    )

    depth = w_query.shape[1]
    rows = depth // dp_size
    q_own = lax.dynamic_slice_in_dim(w_query[0], dp_at * rows, rows, 0)
    kv_own = lax.dynamic_slice_in_dim(w_kv[0], dp_at * rows, rows, 1)
    joined_own = jnp.concatenate([q_own, kv_own[0], kv_own[1]], axis=1)
    joined_own, slabs = lax.optimization_barrier((joined_own, slabs))
    joined_all = lax.all_gather(joined_own, SECTION_DP, axis=0, tiled=True)
    joined_all = joined_all.reshape(sections, depth, -1)

    out_pairs = []
    half = sections // 2
    for pair in range(2):
        block = out_blocks[pair * half : (pair + 1) * half]
        out_pairs.append(lax.all_gather(block, MP_FIRST, axis=1, tiled=True))

    embedded = encode_tiles(patches, vis_gain, vis_bias, slabs, part_at)

    tiles_here = embedded.shape[0] // POOL
    batch_all = tile_batch[0]
    offset_all = tile_offset[0]
    own_batch = lax.dynamic_slice_in_dim(batch_all, section_at * tiles_here, tiles_here, 0)
    capacity = tiles_here // 2
    block_rows = capacity * POOL
    local_ids = jnp.arange(tiles_here, dtype=jnp.int32)
    local_same = (own_batch[:, None] == own_batch[None, :]) & (
        local_ids[None, :] < local_ids[:, None]
    )
    local_rank = jnp.sum(local_same.astype(jnp.int32), axis=1)
    send_rows = jnp.arange(sections * block_rows, dtype=jnp.int32)
    send_target = send_rows // block_rows
    send_rank = send_rows % block_rows // POOL
    send_match = (own_batch[None, :] == send_target[:, None]) & (
        local_rank[None, :] == send_rank[:, None]
    )
    own_rows = jnp.arange(tiles_here * POOL, dtype=jnp.int32)
    send_pick = jnp.repeat(send_match, POOL, axis=1) & (
        (own_rows % POOL)[None, :] == (send_rows % POOL)[:, None]
    )
    blocks = dot(send_pick.astype(jnp.bfloat16), embedded).astype(jnp.bfloat16)
    arrived = exchange(blocks, "section")
    arrived_all = everywhere(arrived, "mp")
    tile_ids = jnp.arange(batch_all.shape[0], dtype=jnp.int32)
    source_ids = tile_ids // tiles_here
    tile_same = (
        (batch_all[:, None] == batch_all[None, :])
        & (source_ids[:, None] == source_ids[None, :])
        & (tile_ids[None, :] < tile_ids[:, None])
    )
    tile_rank = jnp.sum(tile_same.astype(jnp.int32), axis=1)
    slot_rows = jnp.arange(sections * block_rows, dtype=jnp.int32)
    slot_source = slot_rows // block_rows
    slot_rank = slot_rows % block_rows // POOL
    match = (
        (batch_all[None, :] == section_at)
        & (source_ids[None, :] == slot_source[:, None])
        & (tile_rank[None, :] == slot_rank[:, None])
    )
    slot_place = jnp.sum(match.astype(jnp.int32) * offset_all[None, :], axis=1) + slot_rows % POOL
    slot_valid = jnp.any(match, axis=1)
    places = jnp.arange(length, dtype=jnp.int32)
    picker = ((places[:, None] == slot_place[None, :]) & slot_valid[None, :]).astype(jnp.bfloat16)
    covered = jnp.any(
        (batch_all[None, :] == section_at)
        & (places[:, None] >= offset_all[None, :])
        & (places[:, None] < offset_all[None, :] + POOL),
        axis=1,
    )
    image_rows = jnp.concatenate(
        [dot(picker, arrived_all[i]) for i in range(arrived_all.shape[0])], axis=1
    ).astype(jnp.bfloat16)
    state = jnp.where(covered[:, None], image_rows, text_full)

    segment_ids = segments[0, 0]
    allowed = (segment_ids[:, None] == segment_ids[None, :]) & (
        places[None, :] <= places[:, None]
    )
    cosine, sine = rope_tables(length)
    parts = lax.axis_size("mp")
    shard_rows = text.shape[1]
    for layer in range(sections):
        mixed = attend(state, allowed, cosine, sine, gains[layer], joined_all[layer])
        w_full = out_pairs[layer // half][layer % half]
        if layer == sections - 1:
            mine = exchange(mixed.reshape(parts, shard_rows, -1), "mp")
            state = lax.dynamic_slice_in_dim(state, part_at * shard_rows, shard_rows, 0)
        else:
            mine = everywhere(mixed, "mp")
        whole = jnp.concatenate([mine[i] for i in range(parts)], axis=1)
        state = (state.astype(jnp.float32) + dot(whole, w_full)).astype(jnp.bfloat16)

    scaling = float(sections * dp_size * length)
    token_weight = loss_mask.astype(jnp.float32) * scaling / totals.astype(jnp.float32)
    return (state[None], token_weight)


def solution(mesh):
    split = Mesh(
        mesh.devices.reshape(mesh.shape["section"], 4, 2, mesh.shape["mp"]),
        ("section", "dp_0", "dp_1", "mp"),
    )
    return jax.shard_map(
        shards,
        mesh=split,
        in_specs=(
            P("section", DP_MP, None),
            P(SECTION_DP, None),
            P("section", DP, None),
            P("section", DP_MP),
            P(DP, None),
            P(DP, None),
            P("section", None),
            P("section", None, "mp"),
            P("section", None, None, "mp"),
            P("section", "mp", None),
            P(),
            P(),
            P(None, SECTION_DP, "mp"),
            P("mp", SECTION_DP),
            P(SECTION_DP, "mp"),
            P("mp", SECTION_DP),
            P(SECTION_DP, "mp"),
        ),
        out_specs=(P("section", DP_MP, None), P("section", DP_MP)),
        check_vma=False,
    )
```

```python
import jax
import jax.numpy as jnp
from jax import lax
from jax.experimental import pallas as pl
from jax.experimental.pallas import tpu as pltpu
from jax.sharding import Mesh
from jax.sharding import PartitionSpec as P

HD = 128
VHD = 64
GRID = 16
PATCH = 256
POOL = 64
SECTION_DP = ("section", "dp_0", "dp_1")
MP_FIRST = ("mp", "section", "dp_0", "dp_1")
SECTION_DP_MP = ("section", "dp_0", "dp_1", "mp")
DP = ("dp_0", "dp_1")
DP_MP = ("dp_0", "dp_1", "mp")


EPS = 1e-05
ROPE_BASE = 500000.0
BLOCKED = -1e30
ROW_BLOCK = 256
VMEM_LIMIT = 40 * 1024 * 1024


def dot(left, right):
    return jnp.dot(left, right, preferred_element_type=jnp.float32)


def exchange(blocks, axis):
    return lax.all_to_all(blocks, axis, split_axis=0, concat_axis=0, tiled=True)


def everywhere(array, axis):
    return exchange(jnp.broadcast_to(array, (lax.axis_size(axis), *array.shape)), axis)


def shifted(value, axis, steps):
    count = lax.axis_size(axis)
    pairs = [(source, (source + steps) % count) for source in range(count)]
    return lax.ppermute(value, axis, pairs)


def over_axes(array, axes):
    for axis in axes:
        array = lax.psum(array, axis)
    return array


def layer_norm(values, gain, bias):
    wide = values.astype(jnp.float32)
    center = wide - jnp.mean(wide, axis=-1, keepdims=True)
    spread = jnp.mean(center * center, axis=-1, keepdims=True)
    return (center * lax.rsqrt(spread + EPS) * gain + bias).astype(jnp.bfloat16)


def rope_tables(length):
    half = HD // 2
    freqs = ROPE_BASE ** (-2.0 * jnp.arange(half, dtype=jnp.float32) / HD)
    angles = jnp.arange(length, dtype=jnp.float32)[:, None] * freqs[None, :]
    cosine, sine = jnp.cos(angles), jnp.sin(angles)
    return jnp.concatenate([cosine, cosine], axis=1), jnp.concatenate([-sine, sine], axis=1)


def attention_kernel(state_ref, w_ref, cos_ref, sin_ref, seg_col_ref, seg_row_ref, *rest, depth):
    out_refs, (acc_ref, power_ref) = rest[:2], rest[2:]
    step = pl.program_id(0)
    block = state_ref[...]
    wide = block.astype(jnp.float32)
    power = jnp.sum(wide * wide, axis=1, keepdims=True)
    part = dot(block, w_ref[...].reshape(block.shape[1], w_ref.shape[2]))

    @pl.when(step == 0)
    def _():
        acc_ref[...] = part
        power_ref[...] = power

    @pl.when(step > 0)
    def _():
        acc_ref[...] += part
        power_ref[...] += power

    @pl.when(step == pl.num_programs(0) - 1)
    def _():
        heads = acc_ref.shape[1] // HD - 2
        length = acc_ref.shape[0]
        scale = lax.rsqrt(power_ref[...] * (1.0 / depth) + EPS)
        cosine, sine = cos_ref[...], sin_ref[...]

        def column(index):
            return acc_ref[:, index * HD : (index + 1) * HD] * scale

        def rotated(index):
            values = column(index)
            return (values * cosine + pltpu.roll(values, HD // 2, 1) * sine).astype(jnp.bfloat16)

        keyed = rotated(heads)
        valued = column(heads + 1).astype(jnp.bfloat16)
        queries = [rotated(head) for head in range(heads)]
        for begin in range(0, length, ROW_BLOCK):
            end = begin + ROW_BLOCK
            rows = lax.broadcasted_iota(jnp.int32, (ROW_BLOCK, end), 0) + begin
            cols = lax.broadcasted_iota(jnp.int32, (ROW_BLOCK, end), 1)
            allowed = (seg_col_ref[begin:end, :] == seg_row_ref[:, :end]) & (cols <= rows)
            for head in range(heads):
                scores = lax.dot_general(
                    queries[head][begin:end],
                    keyed[:end],
                    (((1,), (1,)), ((), ())),
                    preferred_element_type=jnp.float32,
                ) * HD ** (-0.5)
                scores = jnp.where(allowed, scores, BLOCKED)
                top = jnp.max(scores, axis=1, keepdims=True)
                weights = jnp.exp(scores - top)
                total = jnp.sum(weights, axis=1, keepdims=True)
                mix = dot(weights.astype(jnp.bfloat16), valued[:end]) / total
                side = head * 2 // heads
                at = (head - side * heads // 2) * HD
                out_refs[side][begin:end, at : at + HD] = mix.astype(jnp.bfloat16)


def whole(shape):
    return pl.BlockSpec(shape, lambda *_: (0,) * len(shape))


def params():
    return pltpu.CompilerParams(
        dimension_semantics=("arbitrary",), vmem_limit_bytes=VMEM_LIMIT
    )


def attend(state, slabs, layer, chunks, width, tables, seg_col, seg_row):
    length, depth = state.shape
    steps = chunks // 2
    rows = depth // chunks
    cosine, sine = tables
    heads = width // HD - 2
    half = jax.ShapeDtypeStruct((length, heads * HD // 2), jnp.bfloat16)
    return pl.pallas_call(
        lambda *refs: attention_kernel(*refs, depth=depth),
        grid=(steps,),
        in_specs=[
            pl.BlockSpec((length, 2 * rows), lambda k: (0, k)),
            pl.BlockSpec((2, rows, width), lambda k: (layer * steps + k, 0, 0)),
            whole(cosine.shape),
            whole(sine.shape),
            whole(seg_col.shape),
            whole(seg_row.shape),
        ],
        out_specs=[whole(half.shape), whole(half.shape)],
        out_shape=[half, half],
        scratch_shapes=[
            pltpu.VMEM((length, width), jnp.float32),
            pltpu.VMEM((length, 1), jnp.float32),
        ],
        compiler_params=params(),
        cost_estimate=pl.CostEstimate(
            flops=2 * length * depth * width,
            bytes_accessed=2 * depth * (length + width),
            transcendentals=heads * length * length,
        ),
        name="attend",
    )(state, slabs, cosine, sine, seg_col, seg_row)


def out_kernel(order_ref, *refs, per_block):
    blocks = (len(refs) - 3) // (per_block + 1)
    mixes, weights = refs[: blocks * per_block], refs[blocks * per_block : -3]
    state_ref, out_ref, joined_ref = refs[-3:]

    @pl.when(pl.program_id(0) == 0)
    def _():
        side = joined_ref.shape[2] // per_block
        for at, mix_ref in enumerate(mixes):
            begin = at % per_block * side
            joined_ref[at // per_block, :, begin : begin + side] = mix_ref[...]

    total = state_ref[...].astype(jnp.float32)
    for at, weight_ref in enumerate(weights):
        size = (joined_ref.shape[2], weight_ref.shape[-1])
        total = total + dot(joined_ref[at], weight_ref[...].reshape(size))
    out_ref[...] = total.astype(jnp.bfloat16)


def project_out(mixes, order, pair, layer, state):
    rows, depth = state.shape
    blocks = order.shape[0]
    spread, lines = pair.shape[0], pair.shape[3]
    step_width = 512
    weight_spec = lambda j: pl.BlockSpec(
        (spread, 1, 1, lines, step_width), lambda n, s: (0, s[j], layer, 0, n)
    )
    return pl.pallas_call(
        lambda *refs: out_kernel(*refs, per_block=len(mixes) // blocks),
        grid_spec=pltpu.PrefetchScalarGridSpec(
            num_scalar_prefetch=1,
            grid=(depth // step_width,),
            in_specs=[whole(m.shape) for m in mixes]
            + [weight_spec(j) for j in range(blocks)]
            + [pl.BlockSpec((rows, step_width), lambda n, s: (0, n))],
            out_specs=pl.BlockSpec((rows, step_width), lambda n, s: (0, n)),
            scratch_shapes=[pltpu.VMEM((blocks, rows, spread * lines), jnp.bfloat16)],
        ),
        out_shape=jax.ShapeDtypeStruct((rows, depth), jnp.bfloat16),
        compiler_params=params(),
        cost_estimate=pl.CostEstimate(
            flops=2 * rows * blocks * spread * lines * depth,
            bytes_accessed=2 * depth * (blocks * spread * lines + 2 * rows),
            transcendentals=0,
        ),
        name="project_out",
    )(order, *mixes, *([pair] * blocks), state)


def pack_kernel(at_ref, q_ref, kv_ref, gain_ref, proj_ref, up_ref, down_ref, qkv_ref, out_ref):
    gain = gain_ref[...]
    rows = q_ref.shape[1]
    scaled = lambda block: (block.astype(jnp.float32) * gain).astype(jnp.bfloat16)
    out_ref[:rows, :512] = scaled(q_ref[0])
    out_ref[:rows, 512:640] = scaled(kv_ref[0, 0])
    out_ref[:rows, 640:768] = scaled(kv_ref[0, 1])
    for j in range(4):
        out_ref[j * 128 : (j + 1) * 128, 768:] = proj_ref[:, j * 256 : (j + 1) * 256]
    out_ref[rows : rows + 32] = up_ref[...]
    out_ref[rows + 32 : rows + 64] = down_ref[...]
    for j in range(3):
        out_ref[rows + 64 : rows + 96, j * 256 : (j + 1) * 256] = qkv_ref[j]
    out_ref[rows + 64 : rows + 96, 768:] = jnp.zeros((32, 256), jnp.bfloat16)


def pack(dp_at, dp_size, w_query, w_kv, gain, v_proj, v_up, v_down_t, v_qkv):
    rows = w_query.shape[1] // dp_size
    shape = (rows + 96, 1024)
    return pl.pallas_call(
        pack_kernel,
        grid_spec=pltpu.PrefetchScalarGridSpec(
            num_scalar_prefetch=1,
            grid=(1,),
            in_specs=[
                pl.BlockSpec((1, rows, w_query.shape[2]), lambda n, s: (0, s[0], 0)),
                pl.BlockSpec((1, 2, rows, w_kv.shape[3]), lambda n, s: (0, 0, s[0], 0)),
                pl.BlockSpec((rows, 1), lambda n, s: (s[0], 0)),
            ]
            + [whole(w.shape) for w in (v_proj, v_up, v_down_t, v_qkv)],
            out_specs=whole(shape),
        ),
        out_shape=jax.ShapeDtypeStruct(shape, jnp.bfloat16),
        compiler_params=params(),
        name="pack",
    )(dp_at[None], w_query, w_kv, gain, v_proj, v_up, v_down_t, v_qkv)


def vision_mix_kernel(patches_ref, gain_ref, bias_ref, qkv_ref, out_ref):
    normed = layer_norm(patches_ref[...], gain_ref[...], bias_ref[...])
    weights = qkv_ref[...].reshape(normed.shape[1], qkv_ref.shape[2])
    projected = dot(normed, weights).astype(jnp.bfloat16)
    width = projected.shape[1] // 3
    pair = 2 * VHD
    lower = lax.broadcasted_iota(jnp.int32, (PATCH, pair), 1) < VHD
    for begin in range(0, projected.shape[0], PATCH):
        for at in range(0, width, pair):
            query, keyed, valued = (
                projected[begin : begin + PATCH, i * width + at : i * width + at + pair]
                for i in range(3)
            )
            mixes = []
            for mine in (lower, ~lower):
                scores = lax.dot_general(
                    jnp.where(mine, query, jnp.zeros_like(query)),
                    keyed,
                    (((1,), (1,)), ((), ())),
                    preferred_element_type=jnp.float32,
                ) * VHD ** (-0.5)
                top = jnp.max(scores, axis=1, keepdims=True)
                grown = jnp.exp(scores - top)
                total = jnp.sum(grown, axis=1, keepdims=True)
                mixes.append(dot(grown.astype(jnp.bfloat16), valued) / total)
            mixed = jnp.where(lower, mixes[0], mixes[1])
            out_ref[begin : begin + PATCH, at : at + pair] = mixed.astype(jnp.bfloat16)


def vision_mix(patches, gain, bias, slabs, at):
    width = 768
    return pl.pallas_call(
        vision_mix_kernel,
        grid=(1,),
        in_specs=[
            whole(patches.shape),
            whole(gain.shape),
            whole(bias.shape),
            pl.BlockSpec((slabs.shape[0], 32, width), lambda n: (0, at, 0)),
        ],
        out_specs=whole((patches.shape[0], width // 3)),
        out_shape=jax.ShapeDtypeStruct((patches.shape[0], width // 3), jnp.bfloat16),
        compiler_params=params(),
        name="vision_mix",
    )(patches, gain, bias, slabs)


def vision_hidden_kernel(
    mixed_ref, out_t_ref, patches_ref, gain_ref, bias_ref, up_ref, down_ref, rest_ref, fed_ref
):
    contract_last = (((1,), (1,)), ((), ()))
    wide = mixed_ref.shape[2]
    total = patches_ref[...].astype(jnp.float32)
    for part in range(mixed_ref.shape[0]):
        total = total + lax.dot_general(
            mixed_ref[part],
            out_t_ref[:, part * wide : (part + 1) * wide],
            contract_last,
            preferred_element_type=jnp.float32,
        )
    residual = total.astype(jnp.bfloat16)
    rest_ref[...] = residual
    normed = layer_norm(residual, gain_ref[...], bias_ref[...])
    width = normed.shape[1]
    inner = dot(normed, up_ref[...].reshape(width, width))
    inner = (0.5 * inner * (1.0 + lax.erf(inner * 2.0**-0.5))).astype(jnp.bfloat16)
    fed = lax.dot_general(
        inner,
        down_ref[...].reshape(width, width),
        contract_last,
        preferred_element_type=jnp.float32,
    )
    fed_ref[...] = fed.astype(jnp.bfloat16)


def vision_hidden(gathered, v_out_t, patches, gain, bias, slabs, up_at, down_at):
    width = patches.shape[1]
    block = lambda at: pl.BlockSpec((slabs.shape[0], 32, width), lambda n: (0, at, 0))
    both = jax.ShapeDtypeStruct(patches.shape, jnp.bfloat16)
    return pl.pallas_call(
        vision_hidden_kernel,
        grid=(1,),
        in_specs=[
            whole(gathered.shape),
            whole(v_out_t.shape),
            whole(patches.shape),
            whole(gain.shape),
            whole(bias.shape),
            block(up_at),
            block(down_at),
        ],
        out_specs=[whole(patches.shape), whole(patches.shape)],
        out_shape=[both, both],
        compiler_params=params(),
        name="vision_hidden",
    )(gathered, v_out_t, patches, gain, bias, slabs, slabs)


def pixel_shuffle(states):
    rows, width = states.shape
    side_half = GRID // 2
    arranged = states.reshape(rows // (2 * GRID), 2, side_half, 2, width)
    return arranged.transpose(0, 2, 1, 3, 4).reshape(rows // 4, 4 * width)


def summed_rows(partial):
    blocks = partial.reshape(lax.axis_size("mp"), -1, partial.shape[1])
    return jnp.sum(exchange(blocks, "mp").astype(jnp.float32), axis=0)


def encode_tiles(patches, vis_gain, vis_bias, slabs, v_out_t, part_at):
    proj = [slabs[:, j * 128 : (j + 1) * 128, 768:].reshape(4096, 256) for j in range(4)]
    mixed = vision_mix(patches, vis_gain[:1], vis_bias[:1], slabs, 18)
    residual, fed = vision_hidden(
        everywhere(mixed, "mp"), v_out_t, patches, vis_gain[1:], vis_bias[1:], slabs, 16, 17
    )
    fed = summed_rows(fed)
    own_rows = fed.shape[0]
    own = lax.dynamic_slice_in_dim(residual, part_at * own_rows, own_rows, 0)
    states = (own.astype(jnp.float32) + fed).astype(jnp.bfloat16)
    pooled = everywhere(pixel_shuffle(states), "mp").reshape(-1, 4 * states.shape[1])
    return jnp.concatenate([dot(pooled, block) for block in proj], axis=1).astype(jnp.bfloat16)


def shards(
    text,
    patches,
    segments,
    loss_mask,
    tile_batch,
    tile_offset,
    attn_gain,
    w_query,
    w_kv,
    w_out,
    vis_gain,
    vis_bias,
    v_qkv,
    v_out,
    v_up,
    v_down,
    v_proj,
):
    sections = lax.axis_size("section")
    section_at = lax.axis_index("section")
    part_at = lax.axis_index("mp")
    dp_at = lax.axis_index(DP)
    dp_size = lax.axis_size(DP)
    length = segments.shape[2]

    slab = pack(
        dp_at, dp_size, w_query, w_kv, attn_gain.reshape(-1, 1), v_proj, v_up, v_down.T, v_qkv
    )
    slab, w_out, loss_mask, text, v_out = lax.optimization_barrier(
        (slab, w_out, loss_mask, text, v_out)
    )
    slabs = lax.all_gather(slab, SECTION_DP)

    own_out = w_out[0]
    rows_each = own_out.shape[0] // (sections * dp_size)
    out_blocks = own_out.reshape(sections, dp_size, rows_each, -1)
    out_blocks = lax.dynamic_index_in_dim(out_blocks, dp_at, 1, keepdims=False)
    out_blocks = everywhere(exchange(out_blocks, "section"), "mp")
    out_pairs = []
    half = sections // 2
    for pair in range(2):
        block = out_blocks.reshape(-1, sections, rows_each, own_out.shape[1])
        block = block[:, pair * half : (pair + 1) * half]
        out_pairs.append(lax.all_gather(block, SECTION_DP))

    totals = over_axes(jnp.sum(loss_mask), SECTION_DP_MP)
    text_full = everywhere(text[0], "mp").reshape(length, -1)
    v_out_t = everywhere(v_out.T, "mp").transpose(1, 0, 2).reshape(v_out.shape[1], -1)
    for axis in ("section", "dp_0", "dp_1"):
        v_out_t = everywhere(v_out_t, axis)
    v_out_t = v_out_t.transpose(2, 1, 0, 3, 4).reshape(-1, v_out_t.shape[-1])
    totals, text_full, v_out_t, slabs = lax.optimization_barrier(
        (totals, text_full, v_out_t, slabs)
    )

    embedded = encode_tiles(patches, vis_gain, vis_bias, slabs, v_out_t, part_at)

    tiles_here = embedded.shape[0] // POOL
    batch_all = tile_batch[0]
    offset_all = tile_offset[0]
    own_batch = lax.dynamic_slice_in_dim(batch_all, section_at * tiles_here, tiles_here, 0)
    capacity = tiles_here // 2
    block_rows = capacity * POOL
    local_ids = jnp.arange(tiles_here, dtype=jnp.int32)
    local_same = (own_batch[:, None] == own_batch[None, :]) & (
        local_ids[None, :] < local_ids[:, None]
    )
    local_rank = jnp.sum(local_same.astype(jnp.int32), axis=1)
    send_rows = jnp.arange(sections * block_rows, dtype=jnp.int32)
    send_target = send_rows // block_rows
    send_rank = send_rows % block_rows // POOL
    send_match = (own_batch[None, :] == send_target[:, None]) & (
        local_rank[None, :] == send_rank[:, None]
    )
    own_rows = jnp.arange(tiles_here * POOL, dtype=jnp.int32)
    send_pick = jnp.repeat(send_match, POOL, axis=1) & (
        (own_rows % POOL)[None, :] == (send_rows % POOL)[:, None]
    )
    blocks = dot(send_pick.astype(jnp.bfloat16), embedded).astype(jnp.bfloat16)
    arrived = exchange(blocks, "section")
    arrived_all = everywhere(arrived, "mp")
    tile_ids = jnp.arange(batch_all.shape[0], dtype=jnp.int32)
    source_ids = tile_ids // tiles_here
    tile_same = (
        (batch_all[:, None] == batch_all[None, :])
        & (source_ids[:, None] == source_ids[None, :])
        & (tile_ids[None, :] < tile_ids[:, None])
    )
    tile_rank = jnp.sum(tile_same.astype(jnp.int32), axis=1)
    slot_rows = jnp.arange(sections * block_rows, dtype=jnp.int32)
    slot_source = slot_rows // block_rows
    slot_rank = slot_rows % block_rows // POOL
    match = (
        (batch_all[None, :] == section_at)
        & (source_ids[None, :] == slot_source[:, None])
        & (tile_rank[None, :] == slot_rank[:, None])
    )
    slot_place = jnp.sum(match.astype(jnp.int32) * offset_all[None, :], axis=1) + slot_rows % POOL
    slot_valid = jnp.any(match, axis=1)
    places = jnp.arange(length, dtype=jnp.int32)
    picker = ((places[:, None] == slot_place[None, :]) & slot_valid[None, :]).astype(jnp.bfloat16)
    covered = jnp.any(
        (batch_all[None, :] == section_at)
        & (places[:, None] >= offset_all[None, :])
        & (places[:, None] < offset_all[None, :] + POOL),
        axis=1,
    )
    image_rows = jnp.concatenate(
        [dot(picker, arrived_all[i]) for i in range(arrived_all.shape[0])], axis=1
    ).astype(jnp.bfloat16)
    state = jnp.where(covered[:, None], image_rows, text_full)

    segment_ids = segments[0, 0]
    tables = rope_tables(length)
    parts = lax.axis_size("mp")
    shard_rows = text.shape[1]
    width = w_query.shape[2] + 2 * w_kv.shape[3]
    ring = (part_at + jnp.array([0, 3, 1, 2], jnp.int32)) % parts
    straight = jnp.arange(parts, dtype=jnp.int32)
    for layer in range(sections):
        first, second = attend(
            state,
            slabs,
            layer,
            dp_size,
            width,
            tables,
            segment_ids[:, None],
            segment_ids[None, :],
        )
        pair, at = out_pairs[layer // half], layer % half
        if layer == sections - 1:
            both = jnp.concatenate([first, second], axis=1)
            mine = exchange(both.reshape(parts, shard_rows, -1), "mp")
            state = lax.dynamic_slice_in_dim(state, part_at * shard_rows, shard_rows, 0)
            state = project_out([mine[j] for j in range(parts)], straight, pair, at, state)
        else:
            left_first = shifted(first, "mp", 1)
            right_second = shifted(second, "mp", -1)
            left_second = shifted(second, "mp", 1)
            right_first = shifted(first, "mp", -1)
            far_first = shifted(left_first, "mp", 1)
            far_second = shifted(right_second, "mp", -1)
            mixes = [
                first,
                second,
                left_first,
                left_second,
                right_first,
                right_second,
                far_first,
                far_second,
            ]
            state = project_out(mixes, ring, pair, at, state)

    scaling = float(sections * dp_size * length)
    token_weight = loss_mask.astype(jnp.float32) * scaling / totals.astype(jnp.float32)
    return (state[None], token_weight)


def solution(mesh):
    split = Mesh(
        mesh.devices.reshape(mesh.shape["section"], 4, 2, mesh.shape["mp"]),
        ("section", "dp_0", "dp_1", "mp"),
    )
    return jax.shard_map(
        shards,
        mesh=split,
        in_specs=(
            P("section", DP_MP, None),
            P(SECTION_DP, None),
            P("section", DP, None),
            P("section", DP_MP),
            P(DP, None),
            P(DP, None),
            P("section", None),
            P("section", None, "mp"),
            P("section", None, None, "mp"),
            P("section", "mp", None),
            P(),
            P(),
            P(None, SECTION_DP, "mp"),
            P("mp", SECTION_DP),
            P(SECTION_DP, "mp"),
            P("mp", SECTION_DP),
            P(SECTION_DP, "mp"),
        ),
        out_specs=(P("section", DP_MP, None), P("section", DP_MP)),
        check_vma=False,
    )
```

```python
import jax
import jax.numpy as jnp
from jax import lax
from jax.experimental import pallas as pl
from jax.experimental.pallas import tpu as pltpu
from jax.sharding import Mesh
from jax.sharding import PartitionSpec as P


HD = 128
VHD = 64
GRID = 16
PATCH = 256
POOL = 64
SECTION_DP = ("section", "dp_0", "dp_1")
DP = ("dp_0", "dp_1")
DP_MP = ("dp_0", "dp_1", "mp")


EPS = 1e-05
ROPE_BASE = 500000.0
BLOCKED = -1e30
ROW_BLOCK = 256
SLAB_ROWS = 512
VMEM_LIMIT = 40 * 1024 * 1024


def dot(left, right):
    return jnp.dot(left, right, preferred_element_type=jnp.float32)


def exchange(blocks, axis):
    return lax.all_to_all(blocks, axis, split_axis=0, concat_axis=0, tiled=True)


def everywhere(array, axis):
    return exchange(jnp.broadcast_to(array, (lax.axis_size(axis), *array.shape)), axis)


def shifted(value, axis, steps):
    count = lax.axis_size(axis)
    pairs = [(source, (source + steps) % count) for source in range(count)]
    return lax.ppermute(value, axis, pairs)


def layer_norm(values, gain, bias):
    wide = values.astype(jnp.float32)
    center = wide - jnp.mean(wide, axis=-1, keepdims=True)
    spread = jnp.mean(center * center, axis=-1, keepdims=True)
    return (center * lax.rsqrt(spread + EPS) * gain + bias).astype(jnp.bfloat16)


def rope_tables(length):
    half = HD // 2
    freqs = ROPE_BASE ** (-2.0 * jnp.arange(half, dtype=jnp.float32) / HD)
    angles = jnp.arange(length, dtype=jnp.float32)[:, None] * freqs[None, :]
    cosine, sine = jnp.cos(angles), jnp.sin(angles)
    return jnp.concatenate([cosine, cosine], axis=1), jnp.concatenate([-sine, sine], axis=1)


def attention_kernel(state_ref, w_ref, cos_ref, sin_ref, seg_col_ref, seg_row_ref, *rest, depth):
    out_refs, (acc_ref, power_ref) = rest[:2], rest[2:]
    step = pl.program_id(0)
    block = state_ref[...]
    wide = block.astype(jnp.float32)
    power = jnp.sum(wide * wide, axis=1, keepdims=True)
    part = dot(block, w_ref[...].reshape(block.shape[1], w_ref.shape[2]))

    @pl.when(step == 0)
    def _():
        acc_ref[...] = part
        power_ref[...] = power

    @pl.when(step > 0)
    def _():
        acc_ref[...] += part
        power_ref[...] += power

    @pl.when(step == pl.num_programs(0) - 1)
    def _():
        heads = acc_ref.shape[1] // HD - 2
        length = acc_ref.shape[0]
        scale = lax.rsqrt(power_ref[...] * (1.0 / depth) + EPS)
        cosine, sine = cos_ref[...], sin_ref[...]

        def column(index):
            return acc_ref[:, index * HD : (index + 1) * HD] * scale

        def rotated(index):
            values = column(index)
            return (values * cosine + pltpu.roll(values, HD // 2, 1) * sine).astype(jnp.bfloat16)

        keyed = rotated(heads)
        valued = column(heads + 1).astype(jnp.bfloat16)
        queries = [rotated(head) for head in range(heads)]
        for begin in range(0, length, ROW_BLOCK):
            end = begin + ROW_BLOCK
            rows = lax.broadcasted_iota(jnp.int32, (ROW_BLOCK, end), 0) + begin
            cols = lax.broadcasted_iota(jnp.int32, (ROW_BLOCK, end), 1)
            allowed = (seg_col_ref[begin:end, :] == seg_row_ref[:, :end]) & (cols <= rows)
            for head in range(heads):
                scores = lax.dot_general(
                    queries[head][begin:end],
                    keyed[:end],
                    (((1,), (1,)), ((), ())),
                    preferred_element_type=jnp.float32,
                ) * HD ** (-0.5)
                scores = jnp.where(allowed, scores, BLOCKED)
                top = jnp.max(scores, axis=1, keepdims=True)
                weights = jnp.exp(scores - top)
                total = jnp.sum(weights, axis=1, keepdims=True)
                mix = dot(weights.astype(jnp.bfloat16), valued[:end]) / total
                side = head * 2 // heads
                at = (head - side * heads // 2) * HD
                out_refs[side][begin:end, at : at + HD] = mix.astype(jnp.bfloat16)


def whole(shape):
    return pl.BlockSpec(shape, lambda *_: (0,) * len(shape))


def params():
    return pltpu.CompilerParams(
        dimension_semantics=("arbitrary",), vmem_limit_bytes=VMEM_LIMIT
    )


def state_spec(state, width, index):
    if state.ndim == 2:
        return pl.BlockSpec((state.shape[0], width), lambda n, *s: (0, index(n, *s)))
    per = state.shape[2] // width
    return pl.BlockSpec(
        (None, state.shape[1], width),
        lambda n, *s: (index(n, *s) // per, 0, index(n, *s) % per),
    )


def attend(state, slabs, layer, chunks, width, tables, seg_col, seg_row):
    length = state.shape[-2]
    depth = chunks * SLAB_ROWS
    steps = chunks // 2
    rows = depth // chunks
    cosine, sine = tables
    heads = width // HD - 2
    half = jax.ShapeDtypeStruct((length, heads * HD // 2), jnp.bfloat16)
    return pl.pallas_call(
        lambda *refs: attention_kernel(*refs, depth=depth),
        grid=(steps,),
        in_specs=[
            state_spec(state, 2 * rows, lambda k: k),
            pl.BlockSpec((2, rows, width), lambda k: (layer * steps + k, 0, 0)),
            whole(cosine.shape),
            whole(sine.shape),
            whole(seg_col.shape),
            whole(seg_row.shape),
        ],
        out_specs=[whole(half.shape), whole(half.shape)],
        out_shape=[half, half],
        scratch_shapes=[
            pltpu.VMEM((length, width), jnp.float32),
            pltpu.VMEM((length, 1), jnp.float32),
        ],
        compiler_params=params(),
        cost_estimate=pl.CostEstimate(
            flops=2 * length * depth * width,
            bytes_accessed=2 * depth * (length + width),
            transcendentals=heads * length * length,
        ),
        name="attend",
    )(state, slabs, cosine, sine, seg_col, seg_row)


def out_kernel(order_ref, *refs, per_block):
    blocks = (len(refs) - 3) // (per_block + 1)
    mixes, weights = refs[: blocks * per_block], refs[blocks * per_block : -3]
    state_ref, out_ref, joined_ref = refs[-3:]

    @pl.when(pl.program_id(0) == 0)
    def _():
        side = joined_ref.shape[2] // per_block
        for at, mix_ref in enumerate(mixes):
            begin = at % per_block * side
            joined_ref[at // per_block, :, begin : begin + side] = mix_ref[...]

    total = state_ref[...].astype(jnp.float32)
    for at, weight_ref in enumerate(weights):
        size = (joined_ref.shape[2], weight_ref.shape[-1])
        total = total + dot(joined_ref[at], weight_ref[...].reshape(size))
    out_ref[...] = total.astype(jnp.bfloat16)


def project_out(mixes, order, weights, weight_block, weight_index, state, steps, state_index):
    rows = state.shape[-2]
    width = weight_block[-1]
    per_block = weights.shape[0] * weight_block[-2]
    blocks = 4
    weight_spec = lambda j: pl.BlockSpec(weight_block, lambda n, s: weight_index(n, s[j]))
    return pl.pallas_call(
        lambda *refs: out_kernel(*refs, per_block=len(mixes) // blocks),
        grid_spec=pltpu.PrefetchScalarGridSpec(
            num_scalar_prefetch=1,
            grid=(steps,),
            in_specs=[whole(m.shape) for m in mixes]
            + [weight_spec(j) for j in range(blocks)]
            + [state_spec(state, width, state_index)],
            out_specs=pl.BlockSpec((rows, width), lambda n, s: (0, n)),
            scratch_shapes=[pltpu.VMEM((blocks, rows, per_block), jnp.bfloat16)],
        ),
        out_shape=jax.ShapeDtypeStruct((rows, steps * width), jnp.bfloat16),
        compiler_params=params(),
        cost_estimate=pl.CostEstimate(
            flops=2 * rows * blocks * per_block * steps * width,
            bytes_accessed=2 * steps * width * (blocks * per_block + 2 * rows),
            transcendentals=0,
        ),
        name="project_out",
    )(order, *mixes, *([weights] * blocks), state)


def project_whole(mixes, order, pair, layer, state):
    spread, lines, depth = pair.shape[0], pair.shape[3], pair.shape[4]
    width = 512
    return project_out(
        mixes,
        order,
        pair,
        (spread, 1, 1, lines, width),
        lambda n, block: (0, block, layer, 0, n),
        state,
        depth // width,
        lambda n, s: n,
    )


def project_columns(mixes, order, slabs, state):
    lines, width = 16, 256
    row_at = SLAB_ROWS // lines
    steps = 4
    return project_out(
        mixes,
        order,
        slabs,
        (slabs.shape[0], lines, width),
        lambda n, block: (0, row_at + n // 3 * 4 + block, n % 3),
        state,
        steps,
        lambda n, s: s[4] * steps + n,
    )


def pack_vision_kernel(proj_ref, up_ref, down_ref, qkv_ref, out_t_ref, pack_ref):
    pack_ref[:128] = proj_ref[...]
    pack_ref[128:160] = up_ref[...]
    pack_ref[160:192] = down_ref[...]
    for j in range(3):
        pack_ref[192:224, j * 256 : (j + 1) * 256] = qkv_ref[j]
    pack_ref[192:224, 768:] = jnp.zeros((32, 256), jnp.bfloat16)
    for j in range(4):
        pack_ref[224:256, j * 256 : (j + 1) * 256] = out_t_ref[j]


def pack_vision(*weights):
    shape = (256, 1024)
    return pl.pallas_call(
        pack_vision_kernel,
        grid=(1,),
        in_specs=[whole(w.shape) for w in weights],
        out_specs=whole(shape),
        out_shape=jax.ShapeDtypeStruct(shape, jnp.bfloat16),
        compiler_params=params(),
        name="pack_vision",
    )(*weights)


def pack_kernel(at_ref, q_ref, kv_ref, gain_ref, first_ref, out_ref):
    gain = gain_ref[...]
    rows = q_ref.shape[1]
    scaled = lambda block: (block.astype(jnp.float32) * gain).astype(jnp.bfloat16)
    out_ref[:rows, :512] = scaled(q_ref[0])
    out_ref[:rows, 512:640] = scaled(kv_ref[0, 0])
    out_ref[:rows, 640:768] = scaled(kv_ref[0, 1])
    out_ref[rows + 64 :, 256:] = jnp.zeros((64, 512), jnp.bfloat16)
    for part in range(4):
        at = rows + part * 16
        out_ref[at : at + 16] = first_ref[part, :16, :768]
        out_ref[at + 64 : at + 80, :256] = first_ref[part, :16, 768:]
        begin = 256 + part * 128
        out_ref[rows + 64 : rows + 80, begin : begin + 128] = first_ref[part, 16:, :128]


def pack(dp_at, dp_size, w_query, w_kv, gain, first):
    rows = w_query.shape[1] // dp_size
    shape = (rows + 128, 768)
    return pl.pallas_call(
        pack_kernel,
        grid_spec=pltpu.PrefetchScalarGridSpec(
            num_scalar_prefetch=1,
            grid=(1,),
            in_specs=[
                pl.BlockSpec((1, rows, w_query.shape[2]), lambda n, s: (0, s[0], 0)),
                pl.BlockSpec((1, 2, rows, w_kv.shape[3]), lambda n, s: (0, 0, s[0], 0)),
                pl.BlockSpec((rows, 1), lambda n, s: (s[0], 0)),
                whole(first.shape),
            ],
            out_specs=whole(shape),
        ),
        out_shape=jax.ShapeDtypeStruct(shape, jnp.bfloat16),
        compiler_params=params(),
        name="pack",
    )(dp_at[None], w_query, w_kv, gain, first)


def vision_mix_kernel(patches_ref, gain_ref, bias_ref, qkv_ref, out_ref):
    normed = layer_norm(patches_ref[...], gain_ref[...], bias_ref[...])
    weights = qkv_ref[...].reshape(normed.shape[1], qkv_ref.shape[2])
    projected = dot(normed, weights).astype(jnp.bfloat16)
    width = projected.shape[1] // 3
    pair = 2 * VHD
    lower = lax.broadcasted_iota(jnp.int32, (PATCH, pair), 1) < VHD
    for begin in range(0, projected.shape[0], PATCH):
        for at in range(0, width, pair):
            query, keyed, valued = (
                projected[begin : begin + PATCH, i * width + at : i * width + at + pair]
                for i in range(3)
            )
            mixes = []
            for mine in (lower, ~lower):
                scores = lax.dot_general(
                    jnp.where(mine, query, jnp.zeros_like(query)),
                    keyed,
                    (((1,), (1,)), ((), ())),
                    preferred_element_type=jnp.float32,
                ) * VHD ** (-0.5)
                top = jnp.max(scores, axis=1, keepdims=True)
                grown = jnp.exp(scores - top)
                total = jnp.sum(grown, axis=1, keepdims=True)
                mixes.append(dot(grown.astype(jnp.bfloat16), valued) / total)
            mixed = jnp.where(lower, mixes[0], mixes[1])
            out_ref[begin : begin + PATCH, at : at + pair] = mixed.astype(jnp.bfloat16)


def vision_mix(patches, gain, bias, slabs, at):
    width = 768
    return pl.pallas_call(
        vision_mix_kernel,
        grid=(1,),
        in_specs=[
            whole(patches.shape),
            whole(gain.shape),
            whole(bias.shape),
            pl.BlockSpec((slabs.shape[0], 32, width), lambda n: (0, at, 0)),
        ],
        out_specs=whole((patches.shape[0], width // 3)),
        out_shape=jax.ShapeDtypeStruct((patches.shape[0], width // 3), jnp.bfloat16),
        compiler_params=params(),
        name="vision_mix",
    )(patches, gain, bias, slabs)


def vision_hidden_kernel(
    mixed_ref, out_t_ref, patches_ref, gain_ref, bias_ref, up_ref, down_ref, rest_ref, fed_ref
):
    contract_last = (((1,), (1,)), ((), ()))
    wide = mixed_ref.shape[2]
    out_t = out_t_ref[...].reshape(patches_ref.shape[1], patches_ref.shape[1])
    total = patches_ref[...].astype(jnp.float32)
    for part in range(mixed_ref.shape[0]):
        total = total + lax.dot_general(
            mixed_ref[part],
            out_t[:, part * wide : (part + 1) * wide],
            contract_last,
            preferred_element_type=jnp.float32,
        )
    residual = total.astype(jnp.bfloat16)
    rest_ref[...] = residual
    normed = layer_norm(residual, gain_ref[...], bias_ref[...])
    width = normed.shape[1]
    inner = dot(normed, up_ref[...].reshape(width, width))
    inner = (0.5 * inner * (1.0 + lax.erf(inner * 2.0**-0.5))).astype(jnp.bfloat16)
    fed = lax.dot_general(
        inner,
        down_ref[...].reshape(width, width),
        contract_last,
        preferred_element_type=jnp.float32,
    )
    fed_ref[...] = fed.astype(jnp.bfloat16)


def vision_hidden(gathered, patches, gain, bias, slabs, out_at, up_at, down_at):
    width = patches.shape[1]
    block = lambda at: pl.BlockSpec((slabs.shape[0], 32, width), lambda n: (0, at, 0))
    both = jax.ShapeDtypeStruct(patches.shape, jnp.bfloat16)
    return pl.pallas_call(
        vision_hidden_kernel,
        grid=(1,),
        in_specs=[
            whole(gathered.shape),
            block(out_at),
            whole(patches.shape),
            whole(gain.shape),
            whole(bias.shape),
            block(up_at),
            block(down_at),
        ],
        out_specs=[whole(patches.shape), whole(patches.shape)],
        out_shape=[both, both],
        compiler_params=params(),
        name="vision_hidden",
    )(gathered, slabs, patches, gain, bias, slabs, slabs)


def pixel_shuffle(states):
    rows, width = states.shape
    side_half = GRID // 2
    arranged = states.reshape(rows // (2 * GRID), 2, side_half, 2, width)
    return arranged.transpose(0, 2, 1, 3, 4).reshape(rows // 4, 4 * width)


def summed_rows(partial):
    blocks = partial.reshape(lax.axis_size("mp"), -1, partial.shape[1])
    return jnp.sum(exchange(blocks, "mp").astype(jnp.float32), axis=0)


def encode_tiles(patches, vis_gain, vis_bias, slabs, part_at):
    proj = slabs[:, :128].reshape(-1, slabs.shape[2])
    mixed = vision_mix(patches, vis_gain[:1], vis_bias[:1], slabs, 6)
    residual, fed = vision_hidden(
        everywhere(mixed, "mp"), patches, vis_gain[1:], vis_bias[1:], slabs, 7, 4, 5
    )
    fed = summed_rows(fed)
    own_rows = fed.shape[0]
    own = lax.dynamic_slice_in_dim(residual, part_at * own_rows, own_rows, 0)
    states = (own.astype(jnp.float32) + fed).astype(jnp.bfloat16)
    pooled = everywhere(pixel_shuffle(states), "mp").reshape(-1, 4 * states.shape[1])
    return dot(pooled, proj).astype(jnp.bfloat16)


def shards(
    text,
    patches,
    segments,
    loss_mask,
    tile_batch,
    tile_offset,
    attn_gain,
    w_query,
    w_kv,
    w_out,
    vis_gain,
    vis_bias,
    v_qkv,
    v_out,
    v_up,
    v_down,
    v_proj,
):
    sections = lax.axis_size("section")
    section_at = lax.axis_index("section")
    part_at = lax.axis_index("mp")
    dp_at = lax.axis_index(DP)
    dp_size = lax.axis_size(DP)
    length = segments.shape[2]

    vision_slab = pack_vision(v_proj, v_up, v_down.T, v_qkv, everywhere(v_out.T, "mp"))
    vision_slab, w_out, loss_mask, text, w_query = lax.optimization_barrier(
        (vision_slab, w_out, loss_mask, text, w_query)
    )
    vision_slabs = lax.all_gather(vision_slab, SECTION_DP)

    parts = lax.axis_size("mp")
    own_out = w_out[0]
    depth = own_out.shape[1]
    rows_each = own_out.shape[0] // (sections * dp_size)
    out_blocks = own_out.reshape(sections, dp_size, rows_each, depth)
    out_blocks = lax.dynamic_index_in_dim(out_blocks, dp_at, 1, keepdims=False)
    out_blocks = exchange(out_blocks, "section")
    text_left = shifted(text[0], "mp", 1)
    text_right = shifted(text[0], "mp", -1)
    near = text.shape[1] // 2
    text_far = [
        shifted(text_left[:near], "mp", 1),
        shifted(text_right[near:], "mp", -1),
    ]
    text_full = jnp.zeros((length, depth), text.dtype)
    pieces = ((text[0], 0), (text_left, 6), (text_right, 2), (text_far[0], 4), (text_far[1], 5))
    for piece, ahead in pieces:
        at = (2 * part_at + ahead) % (2 * parts) * near
        text_full = lax.dynamic_update_slice_in_dim(text_full, piece, at, 0)
    first = out_blocks[0].reshape(rows_each, parts, depth // parts).transpose(1, 0, 2)
    count = jnp.sum(loss_mask).astype(jnp.bfloat16)
    first = exchange(
        jnp.concatenate([first, jnp.broadcast_to(count, first.shape)], axis=1), "mp"
    )
    slab = pack(dp_at, dp_size, w_query, w_kv, attn_gain.reshape(-1, 1), first)
    slab, out_blocks = lax.optimization_barrier((slab, out_blocks))
    slabs = lax.all_gather(slab, SECTION_DP)
    own = out_blocks[1:]
    left = shifted(own, "mp", 1)
    right = shifted(own, "mp", -1)
    far = jnp.concatenate([shifted(left[:1], "mp", 1), shifted(right[1:], "mp", -1)], axis=0)
    out_middle = lax.all_gather(
        jnp.stack([own[:2], left[:2], right[:2], far[:2]]), SECTION_DP
    )
    out_last = lax.all_gather(jnp.stack([own[2:], left[2:], right[2:], far[2:]]), SECTION_DP)

    embedded = encode_tiles(patches, vis_gain, vis_bias, vision_slabs, part_at)

    tiles_here = embedded.shape[0] // POOL
    batch_all = tile_batch[0]
    offset_all = tile_offset[0]
    own_batch = lax.dynamic_slice_in_dim(batch_all, section_at * tiles_here, tiles_here, 0)
    capacity = tiles_here // 2
    block_rows = capacity * POOL
    local_ids = jnp.arange(tiles_here, dtype=jnp.int32)
    local_same = (own_batch[:, None] == own_batch[None, :]) & (
        local_ids[None, :] < local_ids[:, None]
    )
    local_rank = jnp.sum(local_same.astype(jnp.int32), axis=1)
    send_rows = jnp.arange(sections * block_rows, dtype=jnp.int32)
    send_target = send_rows // block_rows
    send_rank = send_rows % block_rows // POOL
    send_match = (own_batch[None, :] == send_target[:, None]) & (
        local_rank[None, :] == send_rank[:, None]
    )
    own_rows = jnp.arange(tiles_here * POOL, dtype=jnp.int32)
    send_pick = jnp.repeat(send_match, POOL, axis=1) & (
        (own_rows % POOL)[None, :] == (send_rows % POOL)[:, None]
    )
    blocks = dot(send_pick.astype(jnp.bfloat16), embedded).astype(jnp.bfloat16)
    arrived = exchange(blocks, "section")
    arrived_all = everywhere(arrived, "mp")
    tile_ids = jnp.arange(batch_all.shape[0], dtype=jnp.int32)
    source_ids = tile_ids // tiles_here
    tile_same = (
        (batch_all[:, None] == batch_all[None, :])
        & (source_ids[:, None] == source_ids[None, :])
        & (tile_ids[None, :] < tile_ids[:, None])
    )
    tile_rank = jnp.sum(tile_same.astype(jnp.int32), axis=1)
    slot_rows = jnp.arange(sections * block_rows, dtype=jnp.int32)
    slot_source = slot_rows // block_rows
    slot_rank = slot_rows % block_rows // POOL
    match = (
        (batch_all[None, :] == section_at)
        & (source_ids[None, :] == slot_source[:, None])
        & (tile_rank[None, :] == slot_rank[:, None])
    )
    slot_place = jnp.sum(match.astype(jnp.int32) * offset_all[None, :], axis=1) + slot_rows % POOL
    slot_valid = jnp.any(match, axis=1)
    places = jnp.arange(length, dtype=jnp.int32)
    picker = ((places[:, None] == slot_place[None, :]) & slot_valid[None, :]).astype(jnp.bfloat16)
    covered = jnp.any(
        (batch_all[None, :] == section_at)
        & (places[:, None] >= offset_all[None, :])
        & (places[:, None] < offset_all[None, :] + POOL),
        axis=1,
    )
    image_rows = jnp.concatenate(
        [dot(picker, arrived_all[i]) for i in range(arrived_all.shape[0])], axis=1
    ).astype(jnp.bfloat16)
    state = jnp.where(covered[:, None], image_rows, text_full)

    segment_ids = segments[0, 0]
    tables = rope_tables(length)
    shard_rows = text.shape[1]
    width = w_query.shape[2] + 2 * w_kv.shape[3]
    ring = (part_at + jnp.array([0, 3, 1, 2, 0], jnp.int32)) % parts
    straight = jnp.arange(parts, dtype=jnp.int32)
    ahead = jnp.sum(
        jnp.where((straight[:, None] - part_at - jnp.array([0, 3, 1, 2])) % parts == 0, straight, 0),
        axis=1,
    )
    for layer in range(sections):
        first, second = attend(
            state,
            slabs,
            layer,
            dp_size,
            width,
            tables,
            segment_ids[:, None],
            segment_ids[None, :],
        )
        if layer == sections - 1:
            both = jnp.concatenate([first, second], axis=1)
            mine = exchange(both.reshape(parts, shard_rows, -1), "mp")
            state = lax.dynamic_slice_in_dim(state, part_at * shard_rows, shard_rows, 0)
            state = project_whole([mine[j] for j in range(parts)], ahead, out_last, 0, state)
        else:
            left_first = shifted(first, "mp", 1)
            right_second = shifted(second, "mp", -1)
            left_second = shifted(second, "mp", 1)
            right_first = shifted(first, "mp", -1)
            far_first = shifted(left_first, "mp", 1)
            far_second = shifted(right_second, "mp", -1)
            mixes = [
                first,
                second,
                left_first,
                left_second,
                right_first,
                right_second,
                far_first,
                far_second,
            ]
            if layer == 0:
                state = everywhere(project_columns(mixes, ring, slabs, state), "mp")
            else:
                state = project_whole(mixes, straight, out_middle, layer - 1, state)

    totals = jnp.sum(slabs[:, SLAB_ROWS + 64, 256::128].astype(jnp.float32))
    scaling = float(sections * dp_size * length)
    token_weight = loss_mask.astype(jnp.float32) * scaling / totals
    return (state[None], token_weight)


def solution(mesh):
    split = Mesh(
        mesh.devices.reshape(mesh.shape["section"], 4, 2, mesh.shape["mp"]),
        ("section", "dp_0", "dp_1", "mp"),
    )
    return jax.shard_map(
        shards,
        mesh=split,
        in_specs=(
            P("section", DP_MP, None),
            P(SECTION_DP, None),
            P("section", DP, None),
            P("section", DP_MP),
            P(DP, None),
            P(DP, None),
            P("section", None),
            P("section", None, "mp"),
            P("section", None, None, "mp"),
            P("section", "mp", None),
            P(),
            P(),
            P(None, SECTION_DP, "mp"),
            P("mp", SECTION_DP),
            P(SECTION_DP, "mp"),
            P("mp", SECTION_DP),
            P(SECTION_DP, "mp"),
        ),
        out_specs=(P("section", DP_MP, None), P("section", DP_MP)),
        check_vma=False,
    )
```

```python
import jax
import jax.numpy as jnp
from jax import lax
from jax.experimental import pallas as pl
from jax.experimental.pallas import tpu as pltpu
from jax.sharding import Mesh
from jax.sharding import PartitionSpec as P


HD = 128
VHD = 64
GRID = 16
PATCH = 256
POOL = 64
SECTION_DP = ("section", "dp_0", "dp_1")
DP = ("dp_0", "dp_1")
DP_MP = ("dp_0", "dp_1", "mp")


EPS = 1e-05
ROPE_BASE = 500000.0
BLOCKED = -1e30
ROW_BLOCK = 256
SLAB_ROWS = 512
VMEM_LIMIT = 40 * 1024 * 1024


def dot(left, right):
    return jnp.dot(left, right, preferred_element_type=jnp.float32)


def exchange(blocks, axis):
    return lax.all_to_all(blocks, axis, split_axis=0, concat_axis=0, tiled=True)


def shifted(value, axis, steps):
    count = lax.axis_size(axis)
    pairs = [(source, (source + steps) % count) for source in range(count)]
    return lax.ppermute(value, axis, pairs)


def around(first, second, axis):
    left_first = shifted(first, axis, 1)
    right_second = shifted(second, axis, -1)
    left_second = shifted(second, axis, 1)
    right_first = shifted(first, axis, -1)
    far_first = shifted(left_first, axis, 1)
    far_second = shifted(right_second, axis, -1)
    return (
        (first, second),
        (left_first, left_second),
        (right_first, right_second),
        (far_first, far_second),
    )


def ring_halves(array, axis):
    half = array.shape[0] // 2
    left, right = shifted(array, axis, 1), shifted(array, axis, -1)
    far = (shifted(left[:half], axis, 1), shifted(right[half:], axis, -1))
    return array, left, right, jnp.concatenate(far, axis=0)


def layer_norm(values, gain, bias):
    wide = values.astype(jnp.float32)
    center = wide - jnp.mean(wide, axis=-1, keepdims=True)
    spread = jnp.mean(center * center, axis=-1, keepdims=True)
    return (center * lax.rsqrt(spread + EPS) * gain + bias).astype(jnp.bfloat16)


def rope_tables(length):
    half = HD // 2
    freqs = ROPE_BASE ** (-2.0 * jnp.arange(half, dtype=jnp.float32) / HD)
    angles = jnp.arange(length, dtype=jnp.float32)[:, None] * freqs[None, :]
    cosine, sine = jnp.cos(angles), jnp.sin(angles)
    return jnp.concatenate([cosine, cosine], axis=1), jnp.concatenate([-sine, sine], axis=1)


def attention_kernel(state_ref, w_ref, cos_ref, sin_ref, seg_col_ref, seg_row_ref, *rest, depth):
    out_refs, (acc_ref, power_ref) = rest[:2], rest[2:]
    step = pl.program_id(0)
    block = state_ref[...]
    wide = block.astype(jnp.float32)
    power = jnp.sum(wide * wide, axis=1, keepdims=True)
    part = dot(block, w_ref[...].reshape(block.shape[1], w_ref.shape[2]))

    @pl.when(step == 0)
    def _():
        acc_ref[...] = part
        power_ref[...] = power

    @pl.when(step > 0)
    def _():
        acc_ref[...] += part
        power_ref[...] += power

    @pl.when(step == pl.num_programs(0) - 1)
    def _():
        heads = acc_ref.shape[1] // HD - 2
        length = acc_ref.shape[0]
        scale = lax.rsqrt(power_ref[...] * (1.0 / depth) + EPS)
        cosine, sine = cos_ref[...], sin_ref[...]

        def column(index):
            return acc_ref[:, index * HD : (index + 1) * HD] * scale

        def rotated(index):
            values = column(index)
            return (values * cosine + pltpu.roll(values, HD // 2, 1) * sine).astype(jnp.bfloat16)

        keyed = rotated(heads)
        valued = column(heads + 1).astype(jnp.bfloat16)
        queries = [rotated(head) for head in range(heads)]
        for begin in range(0, length, ROW_BLOCK):
            end = begin + ROW_BLOCK
            rows = lax.broadcasted_iota(jnp.int32, (ROW_BLOCK, end), 0) + begin
            cols = lax.broadcasted_iota(jnp.int32, (ROW_BLOCK, end), 1)
            allowed = (seg_col_ref[begin:end, :] == seg_row_ref[:, :end]) & (cols <= rows)
            for head in range(heads):
                scores = lax.dot_general(
                    queries[head][begin:end],
                    keyed[:end],
                    (((1,), (1,)), ((), ())),
                    preferred_element_type=jnp.float32,
                ) * HD ** (-0.5)
                scores = jnp.where(allowed, scores, BLOCKED)
                top = jnp.max(scores, axis=1, keepdims=True)
                weights = jnp.exp(scores - top)
                total = jnp.sum(weights, axis=1, keepdims=True)
                mix = dot(weights.astype(jnp.bfloat16), valued[:end]) / total
                side = head * 2 // heads
                at = (head - side * heads // 2) * HD
                out_refs[side][begin:end, at : at + HD] = mix.astype(jnp.bfloat16)


def whole(shape):
    return pl.BlockSpec(shape, lambda *_: (0,) * len(shape))


def params():
    return pltpu.CompilerParams(
        dimension_semantics=("arbitrary",), vmem_limit_bytes=VMEM_LIMIT
    )


def state_spec(state, width, index):
    if state.ndim == 2:
        return pl.BlockSpec((state.shape[0], width), lambda n, *s: (0, index(n, *s)))
    per = state.shape[2] // width
    return pl.BlockSpec(
        (None, state.shape[1], width),
        lambda n, *s: (index(n, *s) // per, 0, index(n, *s) % per),
    )


def attend(state, order, slabs, layer, chunks, width, tables, seg_col, seg_row):
    length = state.shape[-2]
    depth = chunks * SLAB_ROWS
    steps = chunks // 2
    rows = depth // chunks
    cosine, sine = tables
    heads = width // HD - 2
    half = jax.ShapeDtypeStruct((length, heads * HD // 2), jnp.bfloat16)
    return pl.pallas_call(
        lambda order_ref, *refs: attention_kernel(*refs, depth=depth),
        grid_spec=pltpu.PrefetchScalarGridSpec(
            num_scalar_prefetch=1,
            grid=(steps,),
            in_specs=[
                state_spec(state, 2 * rows, lambda k, s: k),
                pl.BlockSpec((2, rows, width), lambda k, s: (layer * steps + s[k], 0, 0)),
                whole(cosine.shape),
                whole(sine.shape),
                whole(seg_col.shape),
                whole(seg_row.shape),
            ],
            out_specs=[whole(half.shape), whole(half.shape)],
            scratch_shapes=[
                pltpu.VMEM((length, width), jnp.float32),
                pltpu.VMEM((length, 1), jnp.float32),
            ],
        ),
        out_shape=[half, half],
        compiler_params=params(),
        cost_estimate=pl.CostEstimate(
            flops=2 * length * depth * width,
            bytes_accessed=2 * depth * (length + width),
            transcendentals=heads * length * length,
        ),
        name="attend",
    )(order, state, slabs, cosine, sine, seg_col, seg_row)


def out_kernel(order_ref, *refs, per_block):
    blocks = (len(refs) - 3) // (per_block + 1)
    mixes, weights = refs[: blocks * per_block], refs[blocks * per_block : -3]
    state_ref, out_ref, joined_ref = refs[-3:]

    @pl.when(pl.program_id(0) == 0)
    def _():
        side = joined_ref.shape[2] // per_block
        for at, mix_ref in enumerate(mixes):
            begin = at % per_block * side
            joined_ref[at // per_block, :, begin : begin + side] = mix_ref[...]

    total = state_ref[...].astype(jnp.float32)
    for at, weight_ref in enumerate(weights):
        size = (joined_ref.shape[2], weight_ref.shape[-1])
        total = total + dot(joined_ref[at], weight_ref[...].reshape(size))
    out_ref[...] = total.astype(jnp.bfloat16)


def project_out(mixes, order, weights, weight_block, weight_index, state, steps, state_index):
    rows = state.shape[-2]
    width = weight_block[-1]
    per_block = weights.shape[0] * weight_block[-2]
    blocks = 4
    weight_spec = lambda j: pl.BlockSpec(weight_block, lambda n, s: weight_index(n, s[j]))
    return pl.pallas_call(
        lambda *refs: out_kernel(*refs, per_block=len(mixes) // blocks),
        grid_spec=pltpu.PrefetchScalarGridSpec(
            num_scalar_prefetch=1,
            grid=(steps,),
            in_specs=[whole(m.shape) for m in mixes]
            + [weight_spec(j) for j in range(blocks)]
            + [state_spec(state, width, state_index)],
            out_specs=pl.BlockSpec((rows, width), lambda n, s: (0, n)),
            scratch_shapes=[pltpu.VMEM((blocks, rows, per_block), jnp.bfloat16)],
        ),
        out_shape=jax.ShapeDtypeStruct((rows, steps * width), jnp.bfloat16),
        compiler_params=params(),
        cost_estimate=pl.CostEstimate(
            flops=2 * rows * blocks * per_block * steps * width,
            bytes_accessed=2 * steps * width * (blocks * per_block + 2 * rows),
            transcendentals=0,
        ),
        name="project_out",
    )(order, *mixes, *([weights] * blocks), state)


def project_whole(mixes, order, pair, layer, state):
    spread, lines, depth = pair.shape[0], pair.shape[3], pair.shape[4]
    width = 512
    return project_out(
        mixes,
        order,
        pair,
        (spread, 1, 1, lines, width),
        lambda n, block: (0, block, layer, 0, n),
        state,
        depth // width,
        lambda n, s: s[5 + n // 2] * 2 + n % 2,
    )


def project_columns(mixes, order, slabs, state):
    lines, width = 16, 256
    row_at = SLAB_ROWS // lines
    steps = 4
    return project_out(
        mixes,
        order,
        slabs,
        (slabs.shape[0], lines, width),
        lambda n, block: (
            0,
            row_at + block + n // 3 * (4 + block % 2 - block),
            n % 3 + n // 3 * (block // 2),
        ),
        state,
        steps,
        lambda n, s: n,
    )


def pack_vision_kernel(proj_ref, up_ref, down_ref, qkv_ref, out_t_ref, pack_ref):
    pack_ref[:128] = proj_ref[...]
    pack_ref[128:160] = up_ref[...]
    pack_ref[160:192] = down_ref[...]
    for j in range(3):
        pack_ref[192:224, j * 256 : (j + 1) * 256] = qkv_ref[j]
    pack_ref[192:224, 768:] = jnp.zeros((32, 256), jnp.bfloat16)
    for j in range(4):
        pack_ref[224:256, j * 256 : (j + 1) * 256] = out_t_ref[j]


def pack_vision(*weights):
    shape = (256, 1024)
    return pl.pallas_call(
        pack_vision_kernel,
        grid=(1,),
        in_specs=[whole(w.shape) for w in weights],
        out_specs=whole(shape),
        out_shape=jax.ShapeDtypeStruct(shape, jnp.bfloat16),
        compiler_params=params(),
        name="pack_vision",
    )(*weights)


def pack_kernel(at_ref, q_ref, kv_ref, gain_ref, first_ref, out_ref):
    gain = gain_ref[...]
    rows = q_ref.shape[1]
    scaled = lambda block: (block.astype(jnp.float32) * gain).astype(jnp.bfloat16)
    out_ref[:rows, :512] = scaled(q_ref[0])
    out_ref[:rows, 512:640] = scaled(kv_ref[0, 0])
    out_ref[:rows, 640:768] = scaled(kv_ref[0, 1])
    for part in range(4):
        at = rows + part * 16
        out_ref[at : at + 16] = first_ref[part, :16, :768]
        at, begin = rows + 64 + part % 2 * 16, part // 2 * 256
        out_ref[at : at + 16, begin : begin + 256] = first_ref[part, :16, 768:]
        begin = 512 + part // 2 * 128
        out_ref[at : at + 16, begin : begin + 128] = first_ref[part, 16:, :128]


def pack(dp_at, dp_size, w_query, w_kv, gain, first):
    rows = w_query.shape[1] // dp_size
    shape = (rows + 96, 768)
    return pl.pallas_call(
        pack_kernel,
        grid_spec=pltpu.PrefetchScalarGridSpec(
            num_scalar_prefetch=1,
            grid=(1,),
            in_specs=[
                pl.BlockSpec((1, rows, w_query.shape[2]), lambda n, s: (0, s[0], 0)),
                pl.BlockSpec((1, 2, rows, w_kv.shape[3]), lambda n, s: (0, 0, s[0], 0)),
                pl.BlockSpec((rows, 1), lambda n, s: (s[0], 0)),
                whole(first.shape),
            ],
            out_specs=whole(shape),
        ),
        out_shape=jax.ShapeDtypeStruct(shape, jnp.bfloat16),
        compiler_params=params(),
        name="pack",
    )(dp_at[None], w_query, w_kv, gain, first)


def vision_mix_kernel(patches_ref, gain_ref, bias_ref, qkv_ref, *out_refs):
    normed = layer_norm(patches_ref[...], gain_ref[...], bias_ref[...])
    weights = qkv_ref[...].reshape(normed.shape[1], qkv_ref.shape[2])
    projected = dot(normed, weights).astype(jnp.bfloat16)
    width = projected.shape[1] // 3
    pair = 2 * VHD
    lower = lax.broadcasted_iota(jnp.int32, (PATCH, pair), 1) < VHD
    for begin in range(0, projected.shape[0], PATCH):
        for at in range(0, width, pair):
            query, keyed, valued = (
                projected[begin : begin + PATCH, i * width + at : i * width + at + pair]
                for i in range(3)
            )
            mixes = []
            for mine in (lower, ~lower):
                scores = lax.dot_general(
                    jnp.where(mine, query, jnp.zeros_like(query)),
                    keyed,
                    (((1,), (1,)), ((), ())),
                    preferred_element_type=jnp.float32,
                ) * VHD ** (-0.5)
                top = jnp.max(scores, axis=1, keepdims=True)
                grown = jnp.exp(scores - top)
                total = jnp.sum(grown, axis=1, keepdims=True)
                mixes.append(dot(grown.astype(jnp.bfloat16), valued) / total)
            mixed = jnp.where(lower, mixes[0], mixes[1])
            out_refs[begin // PATCH][:, at : at + pair] = mixed.astype(jnp.bfloat16)


def vision_mix(patches, gain, bias, slabs, at):
    width = 768
    return pl.pallas_call(
        vision_mix_kernel,
        grid=(1,),
        in_specs=[
            whole(patches.shape),
            whole(gain.shape),
            whole(bias.shape),
            pl.BlockSpec((slabs.shape[0], 32, width), lambda n: (0, at, 0)),
        ],
        out_specs=[whole((PATCH, width // 3))] * 2,
        out_shape=[jax.ShapeDtypeStruct((PATCH, width // 3), jnp.bfloat16)] * 2,
        compiler_params=params(),
        name="vision_mix",
    )(patches, gain, bias, slabs)


def vision_hidden_kernel(*refs):
    mixed_refs, rest = refs[:8], refs[8:]
    out_t_ref, patches_ref, gain_ref, bias_ref, up_ref, down_ref, rest_ref, fed_ref = rest
    contract_last = (((1,), (1,)), ((), ()))
    wide = mixed_refs[0].shape[1]
    out_t = out_t_ref[...].reshape(patches_ref.shape[1], patches_ref.shape[1])
    total = patches_ref[...].astype(jnp.float32)
    for part in range(4):
        both = [mixed_refs[2 * part + side][...] for side in range(2)]
        total = total + lax.dot_general(
            jnp.concatenate(both, axis=0),
            out_t[:, part * wide : (part + 1) * wide],
            contract_last,
            preferred_element_type=jnp.float32,
        )
    residual = total.astype(jnp.bfloat16)
    rest_ref[...] = residual
    normed = layer_norm(residual, gain_ref[...], bias_ref[...])
    width = normed.shape[1]
    inner = dot(normed, up_ref[...].reshape(width, width))
    inner = (0.5 * inner * (1.0 + lax.erf(inner * 2.0**-0.5))).astype(jnp.bfloat16)
    fed = lax.dot_general(
        inner,
        down_ref[...].reshape(width, width),
        contract_last,
        preferred_element_type=jnp.float32,
    )
    fed_ref[...] = fed.astype(jnp.bfloat16)


def vision_hidden(gathered, patches, gain, bias, slabs, out_at, up_at, down_at):
    width = patches.shape[1]
    block = lambda at: pl.BlockSpec((slabs.shape[0], 32, width), lambda n: (0, at, 0))
    both = jax.ShapeDtypeStruct(patches.shape, jnp.bfloat16)
    return pl.pallas_call(
        vision_hidden_kernel,
        grid=(1,),
        in_specs=[
            *[whole(part.shape) for part in gathered],
            block(out_at),
            whole(patches.shape),
            whole(gain.shape),
            whole(bias.shape),
            block(up_at),
            block(down_at),
        ],
        out_specs=[whole(patches.shape), whole(patches.shape)],
        out_shape=[both, both],
        compiler_params=params(),
        name="vision_hidden",
    )(*gathered, slabs, patches, gain, bias, slabs, slabs)


def pixel_shuffle(states):
    rows, width = states.shape
    side_half = GRID // 2
    arranged = states.reshape(rows // (2 * GRID), 2, side_half, 2, width)
    return arranged.transpose(0, 2, 1, 3, 4).reshape(rows // 4, 4 * width)


def summed_rows(partial):
    blocks = partial.reshape(lax.axis_size("mp"), -1, partial.shape[1])
    return jnp.sum(exchange(blocks, "mp").astype(jnp.float32), axis=0)


def encode_tiles(patches, vis_gain, vis_bias, slabs, part_at):
    proj = slabs[:, :128].reshape(-1, slabs.shape[2])
    mixed = around(*vision_mix(patches, vis_gain[:1], vis_bias[:1], slabs, 6), "mp")
    residual, fed = vision_hidden(
        [side for pair in mixed for side in pair], patches, vis_gain[1:], vis_bias[1:], slabs, 7, 4, 5
    )
    fed = summed_rows(fed)
    own_rows = fed.shape[0]
    own = lax.dynamic_slice_in_dim(residual, part_at * own_rows, own_rows, 0)
    states = (own.astype(jnp.float32) + fed).astype(jnp.bfloat16)
    pooled = jnp.concatenate(ring_halves(pixel_shuffle(states), "mp"), axis=0)
    return dot(pooled, proj).astype(jnp.bfloat16)


def shards(
    text,
    patches,
    segments,
    loss_mask,
    tile_batch,
    tile_offset,
    attn_gain,
    w_query,
    w_kv,
    w_out,
    vis_gain,
    vis_bias,
    v_qkv,
    v_out,
    v_up,
    v_down,
    v_proj,
):
    sections = lax.axis_size("section")
    section_at = lax.axis_index("section")
    part_at = lax.axis_index("mp")
    dp_at = lax.axis_index(DP)
    dp_size = lax.axis_size(DP)
    length = segments.shape[2]

    out_t = v_out.T
    out_t = jnp.stack([out_t, *(shifted(out_t, "mp", steps) for steps in (1, -1, 2))])
    vision_slab = pack_vision(v_proj, v_up, v_down.T, v_qkv, out_t)
    vision_slab, w_out, loss_mask, text, w_query = lax.optimization_barrier(
        (vision_slab, w_out, loss_mask, text, w_query)
    )
    vision_slabs = lax.all_gather(vision_slab, SECTION_DP)

    parts = lax.axis_size("mp")
    own_out = w_out[0]
    depth = own_out.shape[1]
    rows_each = own_out.shape[0] // (sections * dp_size)
    out_blocks = own_out.reshape(sections, dp_size, rows_each, depth)
    out_blocks = lax.dynamic_index_in_dim(out_blocks, dp_at, 1, keepdims=False)
    out_blocks = exchange(out_blocks, "section")
    text_left = shifted(text[0], "mp", 1)
    text_right = shifted(text[0], "mp", -1)
    near = text.shape[1] // 2
    text_far = [
        shifted(text_left[:near], "mp", 1),
        shifted(text_right[near:], "mp", -1),
    ]
    text_full = jnp.zeros((length, depth), text.dtype)
    pieces = ((text[0], 0), (text_left, 6), (text_right, 2), (text_far[0], 4), (text_far[1], 5))
    for piece, ahead in pieces:
        at = (2 * part_at + ahead) % (2 * parts) * near
        text_full = lax.dynamic_update_slice_in_dim(text_full, piece, at, 0)
    first = out_blocks[0].reshape(rows_each, parts, depth // parts).transpose(1, 0, 2)
    count = jnp.sum(loss_mask).astype(jnp.bfloat16)
    first = exchange(
        jnp.concatenate([first, jnp.broadcast_to(count, first.shape)], axis=1), "mp"
    )
    slab = pack(dp_at, dp_size, w_query, w_kv, attn_gain.reshape(-1, 1), first)
    slab, out_blocks = lax.optimization_barrier((slab, out_blocks))
    slabs = lax.all_gather(slab, SECTION_DP)
    own = out_blocks[1:]
    left = shifted(own, "mp", 1)
    right = shifted(own, "mp", -1)
    far = jnp.concatenate([shifted(left[:1], "mp", 1), shifted(right[1:], "mp", -1)], axis=0)
    out_middle = lax.all_gather(
        jnp.stack([own[:2], left[:2], right[:2], far[:2]]), SECTION_DP
    )
    out_last = lax.all_gather(jnp.stack([own[2:], left[2:], right[2:], far[2:]]), SECTION_DP)

    embedded = encode_tiles(patches, vis_gain, vis_bias, vision_slabs, part_at)

    tiles_here = embedded.shape[0] // POOL
    batch_all = tile_batch[0]
    offset_all = tile_offset[0]
    own_batch = lax.dynamic_slice_in_dim(batch_all, section_at * tiles_here, tiles_here, 0)
    capacity = tiles_here // 2
    block_rows = capacity * POOL
    local_ids = jnp.arange(tiles_here, dtype=jnp.int32)
    local_same = (own_batch[:, None] == own_batch[None, :]) & (
        local_ids[None, :] < local_ids[:, None]
    )
    local_rank = jnp.sum(local_same.astype(jnp.int32), axis=1)
    send_rows = jnp.arange(sections * block_rows, dtype=jnp.int32)
    send_target = (section_at + send_rows // block_rows) % sections
    send_rank = send_rows % block_rows // POOL
    send_match = (own_batch[None, :] == send_target[:, None]) & (
        local_rank[None, :] == send_rank[:, None]
    )
    straight = jnp.arange(parts, dtype=jnp.int32)
    ring = (part_at + jnp.array([0, 3, 1, 2], jnp.int32)) % parts
    each = tiles_here * POOL // parts
    own_rows = (ring[:, None] * each + jnp.arange(each, dtype=jnp.int32)[None, :]).reshape(-1)
    own_tile = jnp.arange(tiles_here, dtype=jnp.int32)[None, :, None] == (own_rows // POOL)
    send_pick = jnp.any(send_match[:, :, None] & own_tile, axis=1) & (
        (own_rows % POOL)[None, :] == (send_rows % POOL)[:, None]
    )
    blocks = dot(send_pick.astype(jnp.bfloat16), embedded).astype(jnp.bfloat16)
    blocks = [blocks[t * block_rows : (t + 1) * block_rows] for t in range(sections)]
    arrived = jnp.concatenate(
        [blocks[0], *(shifted(blocks[t], "section", t) for t in range(1, sections))], axis=0
    )
    arrived_all = ring_halves(arrived, "mp")
    tile_ids = jnp.arange(batch_all.shape[0], dtype=jnp.int32)
    source_ids = tile_ids // tiles_here
    tile_same = (
        (batch_all[:, None] == batch_all[None, :])
        & (source_ids[:, None] == source_ids[None, :])
        & (tile_ids[None, :] < tile_ids[:, None])
    )
    tile_rank = jnp.sum(tile_same.astype(jnp.int32), axis=1)
    slot_rows = jnp.arange(sections * block_rows, dtype=jnp.int32)
    slot_source = (section_at - slot_rows // block_rows) % sections
    slot_rank = slot_rows % block_rows // POOL
    match = (
        (batch_all[None, :] == section_at)
        & (source_ids[None, :] == slot_source[:, None])
        & (tile_rank[None, :] == slot_rank[:, None])
    )
    slot_place = jnp.sum(match.astype(jnp.int32) * offset_all[None, :], axis=1) + slot_rows % POOL
    slot_valid = jnp.any(match, axis=1)
    places = jnp.arange(length, dtype=jnp.int32)
    picker = ((places[:, None] == slot_place[None, :]) & slot_valid[None, :]).astype(jnp.bfloat16)
    covered = jnp.any(
        (batch_all[None, :] == section_at)
        & (places[:, None] >= offset_all[None, :])
        & (places[:, None] < offset_all[None, :] + POOL),
        axis=1,
    )
    columns = depth // parts
    state = jnp.stack(
        [
            jnp.where(
                covered[:, None],
                dot(picker, arrived_all[i]).astype(jnp.bfloat16),
                lax.dynamic_slice_in_dim(text_full, ring[i] * columns, columns, 1),
            )
            for i in range(parts)
        ]
    )

    segment_ids = segments[0, 0]
    tables = rope_tables(length)
    shard_rows = text.shape[1]
    width = w_query.shape[2] + 2 * w_kv.shape[3]
    ahead = jnp.sum(jnp.where(straight[:, None] == ring[None, :], straight[None, :], 0), axis=1)
    filler = jnp.zeros((1,), jnp.int32)
    in_ring = jnp.concatenate([straight, filler, ahead])
    in_order = jnp.concatenate([straight, filler, straight])
    last = jnp.concatenate([ahead, filler, straight])
    for layer in range(sections):
        first, second = attend(
            state,
            ring if layer < 2 else straight,
            slabs,
            layer,
            dp_size,
            width,
            tables,
            segment_ids[:, None],
            segment_ids[None, :],
        )
        if layer == sections - 1:
            both = jnp.concatenate([first, second], axis=1)
            mine = exchange(both.reshape(parts, shard_rows, -1), "mp")
            state = lax.dynamic_slice_in_dim(state, part_at * shard_rows, shard_rows, 0)
            state = project_whole([mine[j] for j in range(parts)], last, out_last, 0, state)
        else:
            mixes = [side for both in around(first, second, "mp") for side in both]
            if layer == 0:
                state = jnp.stack(ring_halves(project_columns(mixes, ring, slabs, state), "mp"))
            else:
                order = in_ring if layer == 1 else in_order
                state = project_whole(mixes, order, out_middle, layer - 1, state)

    counts = slabs[:, SLAB_ROWS + 64 :: 16, 512::128]
    totals = jnp.sum(counts.astype(jnp.float32))
    scaling = float(sections * dp_size * length)
    token_weight = loss_mask.astype(jnp.float32) * scaling / totals
    return (state[None], token_weight)


def solution(mesh):
    split = Mesh(
        mesh.devices.reshape(mesh.shape["section"], 4, 2, mesh.shape["mp"]),
        ("section", "dp_0", "dp_1", "mp"),
    )
    return jax.shard_map(
        shards,
        mesh=split,
        in_specs=(
            P("section", DP_MP, None),
            P(SECTION_DP, None),
            P("section", DP, None),
            P("section", DP_MP),
            P(DP, None),
            P(DP, None),
            P("section", None),
            P("section", None, "mp"),
            P("section", None, None, "mp"),
            P("section", "mp", None),
            P(),
            P(),
            P(None, SECTION_DP, "mp"),
            P("mp", SECTION_DP),
            P(SECTION_DP, "mp"),
            P("mp", SECTION_DP),
            P(SECTION_DP, "mp"),
        ),
        out_specs=(P("section", DP_MP, None), P("section", DP_MP)),
        check_vma=False,
    )
```

```python
import jax
import jax.numpy as jnp
from jax import lax
from jax.experimental import pallas as pl
from jax.experimental.pallas import tpu as pltpu
from jax.sharding import Mesh
from jax.sharding import PartitionSpec as P


HD = 128
VHD = 64
GRID = 16
PATCH = 256
POOL = 64
SECTION_DP = ("section", "dp_0", "dp_1")
DP = ("dp_0", "dp_1")
DP_MP = ("dp_0", "dp_1", "mp")


EPS = 1e-05
ROPE_BASE = 500000.0
BLOCKED = -1e30
ROW_BLOCK = 256
SLAB_ROWS = 512
MIB = 1024 * 1024


def dot(left, right):
    return jnp.dot(left, right, preferred_element_type=jnp.float32)


def exchange(blocks, axis):
    return lax.all_to_all(blocks, axis, split_axis=0, concat_axis=0, tiled=True)


def shifted(value, axis, steps):
    count = lax.axis_size(axis)
    pairs = [(source, (source + steps) % count) for source in range(count)]
    return lax.ppermute(value, axis, pairs)


def around(first, second, axis):
    left_first = shifted(first, axis, 1)
    right_second = shifted(second, axis, -1)
    left_second = shifted(second, axis, 1)
    right_first = shifted(first, axis, -1)
    far_first = shifted(left_first, axis, 1)
    far_second = shifted(right_second, axis, -1)
    return (
        (first, second),
        (left_first, left_second),
        (right_first, right_second),
        (far_first, far_second),
    )


def ring_halves(array, axis):
    half = array.shape[0] // 2
    left, right = shifted(array, axis, 1), shifted(array, axis, -1)
    far = (shifted(left[:half], axis, 1), shifted(right[half:], axis, -1))
    return array, left, right, jnp.concatenate(far, axis=0)


def layer_norm(values, gain, bias):
    wide = values.astype(jnp.float32)
    center = wide - jnp.mean(wide, axis=-1, keepdims=True)
    spread = jnp.mean(center * center, axis=-1, keepdims=True)
    return (center * lax.rsqrt(spread + EPS) * gain + bias).astype(jnp.bfloat16)


def rope_tables(length):
    half = HD // 2
    freqs = ROPE_BASE ** (-2.0 * jnp.arange(half, dtype=jnp.float32) / HD)
    angles = jnp.arange(length, dtype=jnp.float32)[:, None] * freqs[None, :]
    cosine, sine = jnp.cos(angles), jnp.sin(angles)
    return jnp.concatenate([cosine, cosine], axis=1), jnp.concatenate([-sine, sine], axis=1)


def attention_kernel(state_ref, w_ref, cos_ref, sin_ref, seg_col_ref, seg_row_ref, *rest, depth):
    out_refs, (acc_ref, power_ref) = rest[:2], rest[2:]
    step = pl.program_id(0)
    block = state_ref[...]
    wide = block.astype(jnp.float32)
    power = jnp.sum(wide * wide, axis=1, keepdims=True)
    part = dot(block, w_ref[...].reshape(block.shape[1], w_ref.shape[2]))

    @pl.when(step == 0)
    def _():
        acc_ref[...] = part
        power_ref[...] = power

    @pl.when(step > 0)
    def _():
        acc_ref[...] += part
        power_ref[...] += power

    @pl.when(step == pl.num_programs(0) - 1)
    def _():
        heads = acc_ref.shape[1] // HD - 2
        length = acc_ref.shape[0]
        scale = lax.rsqrt(power_ref[...] * (1.0 / depth) + EPS)
        cosine, sine = cos_ref[...], sin_ref[...]

        def column(index):
            return acc_ref[:, index * HD : (index + 1) * HD] * scale

        def rotated(index):
            values = column(index)
            return (values * cosine + pltpu.roll(values, HD // 2, 1) * sine).astype(jnp.bfloat16)

        keyed = rotated(heads)
        valued = column(heads + 1).astype(jnp.bfloat16)
        queries = [rotated(head) for head in range(heads)]
        for begin in range(0, length, ROW_BLOCK):
            end = begin + ROW_BLOCK
            rows = lax.broadcasted_iota(jnp.int32, (ROW_BLOCK, end), 0) + begin
            cols = lax.broadcasted_iota(jnp.int32, (ROW_BLOCK, end), 1)
            allowed = (seg_col_ref[begin:end, :] == seg_row_ref[:, :end]) & (cols <= rows)
            for head in range(heads):
                scores = lax.dot_general(
                    queries[head][begin:end],
                    keyed[:end],
                    (((1,), (1,)), ((), ())),
                    preferred_element_type=jnp.float32,
                ) * HD ** (-0.5)
                scores = jnp.where(allowed, scores, BLOCKED)
                top = jnp.max(scores, axis=1, keepdims=True)
                weights = jnp.exp(scores - top)
                total = jnp.sum(weights, axis=1, keepdims=True)
                mix = dot(weights.astype(jnp.bfloat16), valued[:end]) / total
                side = head * 2 // heads
                at = (head - side * heads // 2) * HD
                out_refs[side][begin:end, at : at + HD] = mix.astype(jnp.bfloat16)


def whole(shape):
    return pl.BlockSpec(shape, lambda *_: (0,) * len(shape))


def params(mib):
    return pltpu.CompilerParams(
        dimension_semantics=("arbitrary",), vmem_limit_bytes=mib * MIB
    )


def state_spec(state, width, index):
    if state.ndim == 2:
        return pl.BlockSpec((state.shape[0], width), lambda n, *s: (0, index(n, *s)))
    per = state.shape[2] // width
    return pl.BlockSpec(
        (None, state.shape[1], width),
        lambda n, *s: (index(n, *s) // per, 0, index(n, *s) % per),
    )


def attend(state, order, slabs, layer, chunks, width, tables, seg_col, seg_row):
    length = state.shape[-2]
    depth = chunks * SLAB_ROWS
    steps = chunks // 2
    rows = depth // chunks
    cosine, sine = tables
    heads = width // HD - 2
    half = jax.ShapeDtypeStruct((length, heads * HD // 2), jnp.bfloat16)
    return pl.pallas_call(
        lambda order_ref, *refs: attention_kernel(*refs, depth=depth),
        grid_spec=pltpu.PrefetchScalarGridSpec(
            num_scalar_prefetch=1,
            grid=(steps,),
            in_specs=[
                state_spec(state, 2 * rows, lambda k, s: k),
                pl.BlockSpec((2, rows, width), lambda k, s: (layer * steps + s[k], 0, 0)),
                whole(cosine.shape),
                whole(sine.shape),
                whole(seg_col.shape),
                whole(seg_row.shape),
            ],
            out_specs=[whole(half.shape), whole(half.shape)],
            scratch_shapes=[
                pltpu.VMEM((length, width), jnp.float32),
                pltpu.VMEM((length, 1), jnp.float32),
            ],
        ),
        out_shape=[half, half],
        compiler_params=params(50),
        cost_estimate=pl.CostEstimate(
            flops=2 * length * depth * width,
            bytes_accessed=2 * depth * (length + width),
            transcendentals=heads * length * length,
        ),
        name="attend",
    )(order, state, slabs, cosine, sine, seg_col, seg_row)


def out_kernel(order_ref, *refs, per_block):
    blocks = (len(refs) - 3) // (per_block + 1)
    mixes, weights = refs[: blocks * per_block], refs[blocks * per_block : -3]
    state_ref, out_ref, joined_ref = refs[-3:]

    @pl.when(pl.program_id(0) == 0)
    def _():
        side = joined_ref.shape[2] // per_block
        for at, mix_ref in enumerate(mixes):
            begin = at % per_block * side
            joined_ref[at // per_block, :, begin : begin + side] = mix_ref[...]

    total = state_ref[...].astype(jnp.float32)
    for at, weight_ref in enumerate(weights):
        size = (joined_ref.shape[2], weight_ref.shape[-1])
        total = total + dot(joined_ref[at], weight_ref[...].reshape(size))
    out_ref[...] = total.astype(jnp.bfloat16)


def project_out(mixes, order, weights, weight_block, weight_index, state, steps, state_index):
    rows = state.shape[-2]
    width = weight_block[-1]
    per_block = weights.shape[0] * weight_block[-2]
    blocks = 4
    weight_spec = lambda j: pl.BlockSpec(weight_block, lambda n, s: weight_index(n, s[j]))
    return pl.pallas_call(
        lambda *refs: out_kernel(*refs, per_block=len(mixes) // blocks),
        grid_spec=pltpu.PrefetchScalarGridSpec(
            num_scalar_prefetch=1,
            grid=(steps,),
            in_specs=[whole(m.shape) for m in mixes]
            + [weight_spec(j) for j in range(blocks)]
            + [state_spec(state, width, state_index)],
            out_specs=pl.BlockSpec((rows, width), lambda n, s: (0, n)),
            scratch_shapes=[pltpu.VMEM((blocks, rows, per_block), jnp.bfloat16)],
        ),
        out_shape=jax.ShapeDtypeStruct((rows, steps * width), jnp.bfloat16),
        compiler_params=params(50),
        cost_estimate=pl.CostEstimate(
            flops=2 * rows * blocks * per_block * steps * width,
            bytes_accessed=2 * steps * width * (blocks * per_block + 2 * rows),
            transcendentals=0,
        ),
        name="project_out",
    )(order, *mixes, *([weights] * blocks), state)


def project_whole(mixes, order, pair, layer, state):
    spread, lines, depth = pair.shape[0], pair.shape[3], pair.shape[4]
    width = 512
    return project_out(
        mixes,
        order,
        pair,
        (spread, 1, 1, lines, width),
        lambda n, block: (0, block, layer, 0, n),
        state,
        depth // width,
        lambda n, s: s[5 + n // 2] * 2 + n % 2,
    )


def project_columns(mixes, order, slabs, state):
    lines, width = 16, 256
    row_at = SLAB_ROWS // lines
    steps = 4
    return project_out(
        mixes,
        order,
        slabs,
        (slabs.shape[0], lines, width),
        lambda n, block: (
            0,
            row_at + block + n // 3 * (4 + block % 2 - block),
            n % 3 + n // 3 * (block // 2),
        ),
        state,
        steps,
        lambda n, s: n,
    )


def pack_kernel(at_ref, q_ref, kv_ref, gain_ref, first_ref, out_ref):
    gain = gain_ref[...]
    rows = q_ref.shape[1]
    scaled = lambda block: (block.astype(jnp.float32) * gain).astype(jnp.bfloat16)
    out_ref[:rows, :512] = scaled(q_ref[0])
    out_ref[:rows, 512:640] = scaled(kv_ref[0, 0])
    out_ref[:rows, 640:768] = scaled(kv_ref[0, 1])
    for part in range(4):
        at = rows + part * 16
        out_ref[at : at + 16] = first_ref[part, :16, :768]
        at, begin = rows + 64 + part % 2 * 16, part // 2 * 256
        out_ref[at : at + 16, begin : begin + 256] = first_ref[part, :16, 768:]
        begin = 512 + part // 2 * 128
        out_ref[at : at + 16, begin : begin + 128] = first_ref[part, 16:, :128]


def pack(dp_at, dp_size, w_query, w_kv, gain, first):
    rows = w_query.shape[1] // dp_size
    shape = (rows + 96, 768)
    return pl.pallas_call(
        pack_kernel,
        grid_spec=pltpu.PrefetchScalarGridSpec(
            num_scalar_prefetch=1,
            grid=(1,),
            in_specs=[
                pl.BlockSpec((1, rows, w_query.shape[2]), lambda n, s: (0, s[0], 0)),
                pl.BlockSpec((1, 2, rows, w_kv.shape[3]), lambda n, s: (0, 0, s[0], 0)),
                pl.BlockSpec((rows, 1), lambda n, s: (s[0], 0)),
                whole(first.shape),
            ],
            out_specs=whole(shape),
        ),
        out_shape=jax.ShapeDtypeStruct(shape, jnp.bfloat16),
        compiler_params=params(56),
        name="pack",
    )(dp_at[None], w_query, w_kv, gain, first)


def vision_mix_kernel(patches_ref, gain_ref, bias_ref, qkv_ref, *out_refs):
    normed = layer_norm(patches_ref[...], gain_ref[...], bias_ref[...])
    weights = qkv_ref[...].reshape(normed.shape[1], qkv_ref.shape[2])
    projected = dot(normed, weights).astype(jnp.bfloat16)
    width = projected.shape[1] // 3
    pair = 2 * VHD
    lower = lax.broadcasted_iota(jnp.int32, (PATCH, pair), 1) < VHD
    for begin in range(0, projected.shape[0], PATCH):
        for at in range(0, width, pair):
            query, keyed, valued = (
                projected[begin : begin + PATCH, i * width + at : i * width + at + pair]
                for i in range(3)
            )
            mixes = []
            for mine in (lower, ~lower):
                scores = lax.dot_general(
                    jnp.where(mine, query, jnp.zeros_like(query)),
                    keyed,
                    (((1,), (1,)), ((), ())),
                    preferred_element_type=jnp.float32,
                ) * VHD ** (-0.5)
                top = jnp.max(scores, axis=1, keepdims=True)
                grown = jnp.exp(scores - top)
                total = jnp.sum(grown, axis=1, keepdims=True)
                mixes.append(dot(grown.astype(jnp.bfloat16), valued) / total)
            mixed = jnp.where(lower, mixes[0], mixes[1])
            out_refs[begin // PATCH][:, at : at + pair] = mixed.astype(jnp.bfloat16)


def vision_mix(patches, gain, bias, slabs, at):
    width = 768
    return pl.pallas_call(
        vision_mix_kernel,
        grid=(1,),
        in_specs=[
            whole(patches.shape),
            whole(gain.shape),
            whole(bias.shape),
            pl.BlockSpec((slabs.shape[0], 32, width), lambda n: (0, at, 0)),
        ],
        out_specs=[whole((PATCH, width // 3))] * 2,
        out_shape=[jax.ShapeDtypeStruct((PATCH, width // 3), jnp.bfloat16)] * 2,
        compiler_params=params(40),
        name="vision_mix",
    )(patches, gain, bias, slabs)


def vision_hidden_kernel(*refs):
    mixed_refs, rest = refs[:8], refs[8:]
    out_t_ref, patches_ref, gain_ref, bias_ref, up_ref, down_ref, rest_ref, fed_ref = rest
    contract_last = (((1,), (1,)), ((), ()))
    wide = mixed_refs[0].shape[1]
    out_t = out_t_ref[...].reshape(patches_ref.shape[1], patches_ref.shape[1])
    total = patches_ref[...].astype(jnp.float32)
    for part in range(4):
        both = [mixed_refs[2 * part + side][...] for side in range(2)]
        total = total + lax.dot_general(
            jnp.concatenate(both, axis=0),
            out_t[:, part * wide : (part + 1) * wide],
            contract_last,
            preferred_element_type=jnp.float32,
        )
    residual = total.astype(jnp.bfloat16)
    rest_ref[...] = residual
    normed = layer_norm(residual, gain_ref[...], bias_ref[...])
    width = normed.shape[1]
    inner = dot(normed, up_ref[...].reshape(width, width))
    inner = (0.5 * inner * (1.0 + lax.erf(inner * 2.0**-0.5))).astype(jnp.bfloat16)
    fed = lax.dot_general(
        inner,
        down_ref[...].reshape(width, width),
        contract_last,
        preferred_element_type=jnp.float32,
    )
    fed_ref[...] = fed.astype(jnp.bfloat16)


def vision_hidden(gathered, patches, gain, bias, slabs, out_at, up_at, down_at):
    width = patches.shape[1]
    block = lambda at: pl.BlockSpec((slabs.shape[0], 32, width), lambda n: (0, at, 0))
    both = jax.ShapeDtypeStruct(patches.shape, jnp.bfloat16)
    return pl.pallas_call(
        vision_hidden_kernel,
        grid=(1,),
        in_specs=[
            *[whole(part.shape) for part in gathered],
            block(out_at),
            whole(patches.shape),
            whole(gain.shape),
            whole(bias.shape),
            block(up_at),
            block(down_at),
        ],
        out_specs=[whole(patches.shape), whole(patches.shape)],
        out_shape=[both, both],
        compiler_params=params(40),
        name="vision_hidden",
    )(*gathered, slabs, patches, gain, bias, slabs, slabs)


def pixel_shuffle(states):
    rows, width = states.shape
    side_half = GRID // 2
    arranged = states.reshape(rows // (2 * GRID), 2, side_half, 2, width)
    return arranged.transpose(0, 2, 1, 3, 4).reshape(rows // 4, 4 * width)


def summed_rows(partial):
    blocks = partial.reshape(lax.axis_size("mp"), -1, partial.shape[1])
    return jnp.sum(exchange(blocks, "mp").astype(jnp.float32), axis=0)


def encode_tiles(patches, vis_gain, vis_bias, slabs, part_at):
    proj = slabs[:, :128].reshape(-1, slabs.shape[2])
    mixed = around(*vision_mix(patches, vis_gain[:1], vis_bias[:1], slabs, 6), "mp")
    residual, fed = vision_hidden(
        [side for pair in mixed for side in pair], patches, vis_gain[1:], vis_bias[1:], slabs, 7, 4, 5
    )
    fed = summed_rows(fed)
    own_rows = fed.shape[0]
    own = lax.dynamic_slice_in_dim(residual, part_at * own_rows, own_rows, 0)
    states = (own.astype(jnp.float32) + fed).astype(jnp.bfloat16)
    pooled = jnp.concatenate(ring_halves(pixel_shuffle(states), "mp"), axis=0)
    return dot(pooled, proj).astype(jnp.bfloat16)


def shards(
    text,
    patches,
    segments,
    loss_mask,
    tile_batch,
    tile_offset,
    attn_gain,
    w_query,
    w_kv,
    w_out,
    vis_gain,
    vis_bias,
    v_qkv,
    v_out,
    v_up,
    v_down,
    v_proj,
):
    sections = lax.axis_size("section")
    section_at = lax.axis_index("section")
    part_at = lax.axis_index("mp")
    dp_at = lax.axis_index(DP)
    dp_size = lax.axis_size(DP)
    length = segments.shape[2]

    out_t = v_out.T
    out_t = jnp.concatenate(
        [out_t, *(shifted(out_t, "mp", steps) for steps in (1, -1, 2))], axis=1
    )
    qkv = jnp.concatenate([*v_qkv, jnp.zeros_like(v_qkv[0])], axis=1)
    vision_slab = jnp.concatenate([v_proj, v_up, v_down.T, qkv, out_t], axis=0)
    vision_slab, w_out, loss_mask, text, w_query = lax.optimization_barrier(
        (vision_slab, w_out, loss_mask, text, w_query)
    )
    vision_slabs = lax.all_gather(vision_slab, SECTION_DP)

    parts = lax.axis_size("mp")
    own_out = w_out[0]
    depth = own_out.shape[1]
    rows_each = own_out.shape[0] // (sections * dp_size)
    out_blocks = own_out.reshape(sections, dp_size, rows_each, depth)
    out_blocks = lax.dynamic_index_in_dim(out_blocks, dp_at, 1, keepdims=False)
    out_blocks = exchange(out_blocks, "section")
    text_left = shifted(text[0], "mp", 1)
    text_right = shifted(text[0], "mp", -1)
    near = text.shape[1] // 2
    text_far = [
        shifted(text_left[:near], "mp", 1),
        shifted(text_right[near:], "mp", -1),
    ]
    text_full = jnp.zeros((length, depth), text.dtype)
    pieces = ((text[0], 0), (text_left, 6), (text_right, 2), (text_far[0], 4), (text_far[1], 5))
    for piece, ahead in pieces:
        at = (2 * part_at + ahead) % (2 * parts) * near
        text_full = lax.dynamic_update_slice_in_dim(text_full, piece, at, 0)
    first = out_blocks[0].reshape(rows_each, parts, depth // parts).transpose(1, 0, 2)
    count = jnp.sum(loss_mask).astype(jnp.bfloat16)
    first = exchange(
        jnp.concatenate([first, jnp.broadcast_to(count, first.shape)], axis=1), "mp"
    )
    slab = pack(dp_at, dp_size, w_query, w_kv, attn_gain.reshape(-1, 1), first)
    slab, out_blocks = lax.optimization_barrier((slab, out_blocks))
    slabs = lax.all_gather(slab, SECTION_DP)
    own = out_blocks[1:]
    left = shifted(own, "mp", 1)
    right = shifted(own, "mp", -1)
    far = jnp.concatenate([shifted(left[:1], "mp", 1), shifted(right[1:], "mp", -1)], axis=0)
    out_middle = lax.all_gather(
        jnp.stack([own[:2], left[:2], right[:2], far[:2]]), SECTION_DP
    )
    out_last = lax.all_gather(jnp.stack([own[2:], left[2:], right[2:], far[2:]]), SECTION_DP)

    embedded = encode_tiles(patches, vis_gain, vis_bias, vision_slabs, part_at)

    tiles_here = embedded.shape[0] // POOL
    batch_all = tile_batch[0]
    offset_all = tile_offset[0]
    own_batch = lax.dynamic_slice_in_dim(batch_all, section_at * tiles_here, tiles_here, 0)
    capacity = tiles_here // 2
    block_rows = capacity * POOL
    local_ids = jnp.arange(tiles_here, dtype=jnp.int32)
    local_same = (own_batch[:, None] == own_batch[None, :]) & (
        local_ids[None, :] < local_ids[:, None]
    )
    local_rank = jnp.sum(local_same.astype(jnp.int32), axis=1)
    send_rows = jnp.arange(sections * block_rows, dtype=jnp.int32)
    send_target = (section_at + send_rows // block_rows) % sections
    send_rank = send_rows % block_rows // POOL
    send_match = (own_batch[None, :] == send_target[:, None]) & (
        local_rank[None, :] == send_rank[:, None]
    )
    straight = jnp.arange(parts, dtype=jnp.int32)
    ring = (part_at + jnp.array([0, 3, 1, 2], jnp.int32)) % parts
    each = tiles_here * POOL // parts
    own_rows = (ring[:, None] * each + jnp.arange(each, dtype=jnp.int32)[None, :]).reshape(-1)
    own_tile = jnp.arange(tiles_here, dtype=jnp.int32)[None, :, None] == (own_rows // POOL)
    send_pick = jnp.any(send_match[:, :, None] & own_tile, axis=1) & (
        (own_rows % POOL)[None, :] == (send_rows % POOL)[:, None]
    )
    blocks = dot(send_pick.astype(jnp.bfloat16), embedded).astype(jnp.bfloat16)
    blocks = [blocks[t * block_rows : (t + 1) * block_rows] for t in range(sections)]
    arrived = jnp.concatenate(
        [blocks[0], *(shifted(blocks[t], "section", t) for t in range(1, sections))], axis=0
    )
    arrived_all = ring_halves(arrived, "mp")
    tile_ids = jnp.arange(batch_all.shape[0], dtype=jnp.int32)
    source_ids = tile_ids // tiles_here
    tile_same = (
        (batch_all[:, None] == batch_all[None, :])
        & (source_ids[:, None] == source_ids[None, :])
        & (tile_ids[None, :] < tile_ids[:, None])
    )
    tile_rank = jnp.sum(tile_same.astype(jnp.int32), axis=1)
    slot_rows = jnp.arange(sections * block_rows, dtype=jnp.int32)
    slot_source = (section_at - slot_rows // block_rows) % sections
    slot_rank = slot_rows % block_rows // POOL
    match = (
        (batch_all[None, :] == section_at)
        & (source_ids[None, :] == slot_source[:, None])
        & (tile_rank[None, :] == slot_rank[:, None])
    )
    slot_place = jnp.sum(match.astype(jnp.int32) * offset_all[None, :], axis=1) + slot_rows % POOL
    slot_valid = jnp.any(match, axis=1)
    places = jnp.arange(length, dtype=jnp.int32)
    picker = ((places[:, None] == slot_place[None, :]) & slot_valid[None, :]).astype(jnp.bfloat16)
    covered = jnp.any(
        (batch_all[None, :] == section_at)
        & (places[:, None] >= offset_all[None, :])
        & (places[:, None] < offset_all[None, :] + POOL),
        axis=1,
    )
    columns = depth // parts
    state = jnp.stack(
        [
            jnp.where(
                covered[:, None],
                dot(picker, arrived_all[i]).astype(jnp.bfloat16),
                lax.dynamic_slice_in_dim(text_full, ring[i] * columns, columns, 1),
            )
            for i in range(parts)
        ]
    )

    segment_ids = segments[0, 0]
    tables = rope_tables(length)
    shard_rows = text.shape[1]
    width = w_query.shape[2] + 2 * w_kv.shape[3]
    ahead = jnp.sum(jnp.where(straight[:, None] == ring[None, :], straight[None, :], 0), axis=1)
    filler = jnp.zeros((1,), jnp.int32)
    in_ring = jnp.concatenate([straight, filler, ahead])
    in_order = jnp.concatenate([straight, filler, straight])
    last = jnp.concatenate([ahead, filler, straight])
    for layer in range(sections):
        first, second = attend(
            state,
            ring if layer < 2 else straight,
            slabs,
            layer,
            dp_size,
            width,
            tables,
            segment_ids[:, None],
            segment_ids[None, :],
        )
        if layer == sections - 1:
            both = jnp.concatenate([first, second], axis=1)
            mine = exchange(both.reshape(parts, shard_rows, -1), "mp")
            state = lax.dynamic_slice_in_dim(state, part_at * shard_rows, shard_rows, 0)
            state = project_whole([mine[j] for j in range(parts)], last, out_last, 0, state)
        else:
            mixes = [side for both in around(first, second, "mp") for side in both]
            if layer == 0:
                state = jnp.stack(ring_halves(project_columns(mixes, ring, slabs, state), "mp"))
            else:
                order = in_ring if layer == 1 else in_order
                state = project_whole(mixes, order, out_middle, layer - 1, state)

    counts = slabs[:, SLAB_ROWS + 64 :: 16, 512::128]
    totals = jnp.sum(counts.astype(jnp.float32))
    scaling = float(sections * dp_size * length)
    token_weight = loss_mask.astype(jnp.float32) * scaling / totals
    return (state[None], token_weight)


def solution(mesh):
    split = Mesh(
        mesh.devices.reshape(mesh.shape["section"], 4, 2, mesh.shape["mp"]),
        ("section", "dp_0", "dp_1", "mp"),
    )
    return jax.shard_map(
        shards,
        mesh=split,
        in_specs=(
            P("section", DP_MP, None),
            P(SECTION_DP, None),
            P("section", DP, None),
            P("section", DP_MP),
            P(DP, None),
            P(DP, None),
            P("section", None),
            P("section", None, "mp"),
            P("section", None, None, "mp"),
            P("section", "mp", None),
            P(),
            P(),
            P(None, SECTION_DP, "mp"),
            P("mp", SECTION_DP),
            P(SECTION_DP, "mp"),
            P("mp", SECTION_DP),
            P(SECTION_DP, "mp"),
        ),
        out_specs=(P("section", DP_MP, None), P("section", DP_MP)),
        check_vma=False,
    )
```

```python
import jax
import jax.numpy as jnp
from jax import lax
from jax.experimental import pallas as pl
from jax.experimental.pallas import tpu as pltpu
from jax.sharding import Mesh
from jax.sharding import PartitionSpec as P


HD = 128
VHD = 64
GRID = 16
PATCH = 256
POOL = 64
SECTION_DP = ("section", "dp_0", "dp_1")
DP = ("dp_0", "dp_1")
DP_MP = ("dp_0", "dp_1", "mp")


EPS = 1e-05
ROPE_BASE = 500000.0
BLOCKED = -1e30
ROW_BLOCK = 256
SLAB_ROWS = 512
MIB = 1024 * 1024


def dot(left, right):
    return jnp.dot(left, right, preferred_element_type=jnp.float32)


def exchange(blocks, axis):
    return lax.all_to_all(blocks, axis, split_axis=0, concat_axis=0, tiled=True)


def shifted(value, axis, steps):
    count = lax.axis_size(axis)
    pairs = [(source, (source + steps) % count) for source in range(count)]
    return lax.ppermute(value, axis, pairs)


def around(first, second, axis):
    left_first = shifted(first, axis, 1)
    right_second = shifted(second, axis, -1)
    left_second = shifted(second, axis, 1)
    right_first = shifted(first, axis, -1)
    far_first = shifted(left_first, axis, 1)
    far_second = shifted(right_second, axis, -1)
    return (
        (first, second),
        (left_first, left_second),
        (right_first, right_second),
        (far_first, far_second),
    )


def ring_halves(array, axis):
    half = array.shape[0] // 2
    left, right = shifted(array, axis, 1), shifted(array, axis, -1)
    far = (shifted(left[:half], axis, 1), shifted(right[half:], axis, -1))
    return array, left, right, jnp.concatenate(far, axis=0)


def layer_norm(values, gain, bias):
    wide = values.astype(jnp.float32)
    center = wide - jnp.mean(wide, axis=-1, keepdims=True)
    spread = jnp.mean(center * center, axis=-1, keepdims=True)
    return (center * lax.rsqrt(spread + EPS) * gain + bias).astype(jnp.bfloat16)


def rope_tables(length):
    half = HD // 2
    freqs = ROPE_BASE ** (-2.0 * jnp.arange(half, dtype=jnp.float32) / HD)
    angles = jnp.arange(length, dtype=jnp.float32)[:, None] * freqs[None, :]
    cosine, sine = jnp.cos(angles), jnp.sin(angles)
    return jnp.concatenate([cosine, cosine], axis=1), jnp.concatenate([-sine, sine], axis=1)


def attention_kernel(state_ref, w_ref, cos_ref, sin_ref, seg_col_ref, seg_row_ref, *rest, depth):
    out_refs, (acc_ref, power_ref) = rest[:2], rest[2:]
    step = pl.program_id(0)
    block = state_ref[...]
    wide = block.astype(jnp.float32)
    power = jnp.sum(wide * wide, axis=1, keepdims=True)
    part = dot(block, w_ref[...].reshape(block.shape[1], w_ref.shape[2]))

    @pl.when(step == 0)
    def _():
        acc_ref[...] = part
        power_ref[...] = power

    @pl.when(step > 0)
    def _():
        acc_ref[...] += part
        power_ref[...] += power

    @pl.when(step == pl.num_programs(0) - 1)
    def _():
        heads = acc_ref.shape[1] // HD - 2
        length = acc_ref.shape[0]
        scale = lax.rsqrt(power_ref[...] * (1.0 / depth) + EPS)
        cosine, sine = cos_ref[...], sin_ref[...]

        def column(index):
            return acc_ref[:, index * HD : (index + 1) * HD] * scale

        def rotated(index):
            values = column(index)
            return (values * cosine + pltpu.roll(values, HD // 2, 1) * sine).astype(jnp.bfloat16)

        keyed = rotated(heads)
        valued = column(heads + 1).astype(jnp.bfloat16)
        queries = [rotated(head) for head in range(heads)]
        for begin in range(0, length, ROW_BLOCK):
            end = begin + ROW_BLOCK
            rows = lax.broadcasted_iota(jnp.int32, (ROW_BLOCK, end), 0) + begin
            cols = lax.broadcasted_iota(jnp.int32, (ROW_BLOCK, end), 1)
            allowed = (seg_col_ref[begin:end, :] == seg_row_ref[:, :end]) & (cols <= rows)
            for head in range(heads):
                scores = lax.dot_general(
                    queries[head][begin:end],
                    keyed[:end],
                    (((1,), (1,)), ((), ())),
                    preferred_element_type=jnp.float32,
                ) * HD ** (-0.5)
                scores = jnp.where(allowed, scores, BLOCKED)
                top = jnp.max(scores, axis=1, keepdims=True)
                weights = jnp.exp(scores - top)
                total = jnp.sum(weights, axis=1, keepdims=True)
                mix = dot(weights.astype(jnp.bfloat16), valued[:end]) / total
                side = head * 2 // heads
                at = (head - side * heads // 2) * HD
                out_refs[side][begin:end, at : at + HD] = mix.astype(jnp.bfloat16)


def whole(shape):
    return pl.BlockSpec(shape, lambda *_: (0,) * len(shape))


def params(mib):
    return pltpu.CompilerParams(
        dimension_semantics=("arbitrary",), vmem_limit_bytes=mib * MIB
    )


def state_spec(state, width, index):
    if state.ndim == 2:
        return pl.BlockSpec((state.shape[0], width), lambda n, *s: (0, index(n, *s)))
    per = state.shape[2] // width
    return pl.BlockSpec(
        (None, state.shape[1], width),
        lambda n, *s: (index(n, *s) // per, 0, index(n, *s) % per),
    )


def attend(state, order, slabs, layer, chunks, width, tables, seg_col, seg_row):
    length = state.shape[-2]
    depth = chunks * SLAB_ROWS
    steps = chunks // 2
    rows = depth // chunks
    cosine, sine = tables
    heads = width // HD - 2
    half = jax.ShapeDtypeStruct((length, heads * HD // 2), jnp.bfloat16)
    return pl.pallas_call(
        lambda order_ref, *refs: attention_kernel(*refs, depth=depth),
        grid_spec=pltpu.PrefetchScalarGridSpec(
            num_scalar_prefetch=1,
            grid=(steps,),
            in_specs=[
                state_spec(state, 2 * rows, lambda k, s: k),
                pl.BlockSpec((2, rows, width), lambda k, s: (layer * steps + s[k], 0, 0)),
                whole(cosine.shape),
                whole(sine.shape),
                whole(seg_col.shape),
                whole(seg_row.shape),
            ],
            out_specs=[whole(half.shape), whole(half.shape)],
            scratch_shapes=[
                pltpu.VMEM((length, width), jnp.float32),
                pltpu.VMEM((length, 1), jnp.float32),
            ],
        ),
        out_shape=[half, half],
        compiler_params=params(50),
        cost_estimate=pl.CostEstimate(
            flops=2 * length * depth * width,
            bytes_accessed=2 * depth * (length + width),
            transcendentals=heads * length * length,
        ),
        name="attend",
    )(order, state, slabs, cosine, sine, seg_col, seg_row)


def out_kernel(order_ref, *refs, per_block):
    blocks = (len(refs) - 3) // (per_block + 1)
    mixes, weights = refs[: blocks * per_block], refs[blocks * per_block : -3]
    state_ref, out_ref, joined_ref = refs[-3:]

    @pl.when(pl.program_id(0) == 0)
    def _():
        side = joined_ref.shape[2] // per_block
        for at, mix_ref in enumerate(mixes):
            begin = at % per_block * side
            joined_ref[at // per_block, :, begin : begin + side] = mix_ref[...]

    total = state_ref[...].astype(jnp.float32)
    for at, weight_ref in enumerate(weights):
        size = (joined_ref.shape[2], weight_ref.shape[-1])
        total = total + dot(joined_ref[at], weight_ref[...].reshape(size))
    out_ref[...] = total.astype(jnp.bfloat16)


def project_out(mixes, order, weights, weight_block, weight_index, state, steps, state_index):
    rows = state.shape[-2]
    width = weight_block[-1]
    per_block = weights.shape[0] * weight_block[-2]
    blocks = 4
    weight_spec = lambda j: pl.BlockSpec(weight_block, lambda n, s: weight_index(n, s[j]))
    return pl.pallas_call(
        lambda *refs: out_kernel(*refs, per_block=len(mixes) // blocks),
        grid_spec=pltpu.PrefetchScalarGridSpec(
            num_scalar_prefetch=1,
            grid=(steps,),
            in_specs=[whole(m.shape) for m in mixes]
            + [weight_spec(j) for j in range(blocks)]
            + [state_spec(state, width, state_index)],
            out_specs=pl.BlockSpec((rows, width), lambda n, s: (0, n)),
            scratch_shapes=[pltpu.VMEM((blocks, rows, per_block), jnp.bfloat16)],
        ),
        out_shape=jax.ShapeDtypeStruct((rows, steps * width), jnp.bfloat16),
        compiler_params=params(50),
        cost_estimate=pl.CostEstimate(
            flops=2 * rows * blocks * per_block * steps * width,
            bytes_accessed=2 * steps * width * (blocks * per_block + 2 * rows),
            transcendentals=0,
        ),
        name="project_out",
    )(order, *mixes, *([weights] * blocks), state)


def project_whole(mixes, order, pair, layer, state):
    spread, lines, depth = pair.shape[0], pair.shape[3], pair.shape[4]
    width = 1024
    return project_out(
        mixes,
        order,
        pair,
        (spread, 1, 1, lines, width),
        lambda n, block: (0, block, layer, 0, n),
        state,
        depth // width,
        lambda n, s: s[5 + n],
    )


def project_columns(mixes, order, slabs, state):
    lines, width = 16, 256
    row_at = SLAB_ROWS // lines
    steps = 4
    return project_out(
        mixes,
        order,
        slabs,
        (slabs.shape[0], lines, width),
        lambda n, block: (
            0,
            row_at + block + n // 3 * (4 + block % 2 - block),
            n % 3 + n // 3 * (block // 2),
        ),
        state,
        steps,
        lambda n, s: n,
    )


def pack_kernel(at_ref, q_ref, kv_ref, gain_ref, first_ref, out_ref):
    gain = gain_ref[...]
    rows = q_ref.shape[1]
    scaled = lambda block: (block.astype(jnp.float32) * gain).astype(jnp.bfloat16)
    out_ref[:rows, :512] = scaled(q_ref[0])
    out_ref[:rows, 512:640] = scaled(kv_ref[0, 0])
    out_ref[:rows, 640:768] = scaled(kv_ref[0, 1])
    for part in range(4):
        at = rows + part * 16
        out_ref[at : at + 16] = first_ref[part, :16, :768]
        at, begin = rows + 64 + part % 2 * 16, part // 2 * 256
        out_ref[at : at + 16, begin : begin + 256] = first_ref[part, :16, 768:]
        begin = 512 + part // 2 * 128
        out_ref[at : at + 16, begin : begin + 128] = first_ref[part, 16:, :128]


def pack(dp_at, dp_size, w_query, w_kv, gain, first):
    rows = w_query.shape[1] // dp_size
    shape = (rows + 96, 768)
    return pl.pallas_call(
        pack_kernel,
        grid_spec=pltpu.PrefetchScalarGridSpec(
            num_scalar_prefetch=1,
            grid=(1,),
            in_specs=[
                pl.BlockSpec((1, rows, w_query.shape[2]), lambda n, s: (0, s[0], 0)),
                pl.BlockSpec((1, 2, rows, w_kv.shape[3]), lambda n, s: (0, 0, s[0], 0)),
                pl.BlockSpec((rows, 1), lambda n, s: (s[0], 0)),
                whole(first.shape),
            ],
            out_specs=whole(shape),
        ),
        out_shape=jax.ShapeDtypeStruct(shape, jnp.bfloat16),
        compiler_params=params(56),
        name="pack",
    )(dp_at[None], w_query, w_kv, gain, first)


def vision_mix_kernel(patches_ref, gain_ref, bias_ref, qkv_ref, *out_refs):
    normed = layer_norm(patches_ref[...], gain_ref[...], bias_ref[...])
    weights = qkv_ref[...].reshape(normed.shape[1], qkv_ref.shape[2])
    projected = dot(normed, weights).astype(jnp.bfloat16)
    width = projected.shape[1] // 3
    pair = 2 * VHD
    lower = lax.broadcasted_iota(jnp.int32, (PATCH, pair), 1) < VHD
    for begin in range(0, projected.shape[0], PATCH):
        for at in range(0, width, pair):
            query, keyed, valued = (
                projected[begin : begin + PATCH, i * width + at : i * width + at + pair]
                for i in range(3)
            )
            mixes = []
            for mine in (lower, ~lower):
                scores = lax.dot_general(
                    jnp.where(mine, query, jnp.zeros_like(query)),
                    keyed,
                    (((1,), (1,)), ((), ())),
                    preferred_element_type=jnp.float32,
                ) * VHD ** (-0.5)
                top = jnp.max(scores, axis=1, keepdims=True)
                grown = jnp.exp(scores - top)
                total = jnp.sum(grown, axis=1, keepdims=True)
                mixes.append(dot(grown.astype(jnp.bfloat16), valued) / total)
            mixed = jnp.where(lower, mixes[0], mixes[1])
            out_refs[begin // PATCH][:, at : at + pair] = mixed.astype(jnp.bfloat16)


def vision_mix(patches, gain, bias, slabs, at):
    width = 768
    return pl.pallas_call(
        vision_mix_kernel,
        grid=(1,),
        in_specs=[
            whole(patches.shape),
            whole(gain.shape),
            whole(bias.shape),
            pl.BlockSpec((slabs.shape[0], 32, width), lambda n: (0, at, 0)),
        ],
        out_specs=[whole((PATCH, width // 3))] * 2,
        out_shape=[jax.ShapeDtypeStruct((PATCH, width // 3), jnp.bfloat16)] * 2,
        compiler_params=params(40),
        name="vision_mix",
    )(patches, gain, bias, slabs)


def vision_hidden_kernel(*refs):
    mixed_refs, rest = refs[:8], refs[8:]
    out_t_ref, patches_ref, gain_ref, bias_ref, up_ref, down_ref, rest_ref, fed_ref = rest
    contract_last = (((1,), (1,)), ((), ()))
    wide = mixed_refs[0].shape[1]
    out_t = out_t_ref[...].reshape(patches_ref.shape[1], patches_ref.shape[1])
    total = patches_ref[...].astype(jnp.float32)
    for part in range(4):
        both = [mixed_refs[2 * part + side][...] for side in range(2)]
        total = total + lax.dot_general(
            jnp.concatenate(both, axis=0),
            out_t[:, part * wide : (part + 1) * wide],
            contract_last,
            preferred_element_type=jnp.float32,
        )
    residual = total.astype(jnp.bfloat16)
    rest_ref[...] = residual
    normed = layer_norm(residual, gain_ref[...], bias_ref[...])
    width = normed.shape[1]
    inner = dot(normed, up_ref[...].reshape(width, width))
    inner = (0.5 * inner * (1.0 + lax.erf(inner * 2.0**-0.5))).astype(jnp.bfloat16)
    fed = lax.dot_general(
        inner,
        down_ref[...].reshape(width, width),
        contract_last,
        preferred_element_type=jnp.float32,
    )
    fed_ref[...] = fed.astype(jnp.bfloat16)


def vision_hidden(gathered, patches, gain, bias, slabs, out_at, up_at, down_at):
    width = patches.shape[1]
    block = lambda at: pl.BlockSpec((slabs.shape[0], 32, width), lambda n: (0, at, 0))
    both = jax.ShapeDtypeStruct(patches.shape, jnp.bfloat16)
    return pl.pallas_call(
        vision_hidden_kernel,
        grid=(1,),
        in_specs=[
            *[whole(part.shape) for part in gathered],
            block(out_at),
            whole(patches.shape),
            whole(gain.shape),
            whole(bias.shape),
            block(up_at),
            block(down_at),
        ],
        out_specs=[whole(patches.shape), whole(patches.shape)],
        out_shape=[both, both],
        compiler_params=params(40),
        name="vision_hidden",
    )(*gathered, slabs, patches, gain, bias, slabs, slabs)


def pixel_shuffle(states):
    rows, width = states.shape
    side_half = GRID // 2
    arranged = states.reshape(rows // (2 * GRID), 2, side_half, 2, width)
    return arranged.transpose(0, 2, 1, 3, 4).reshape(rows // 4, 4 * width)


def summed_rows(partial):
    blocks = partial.reshape(lax.axis_size("mp"), -1, partial.shape[1])
    return jnp.sum(exchange(blocks, "mp").astype(jnp.float32), axis=0)


def encode_tiles(patches, vis_gain, vis_bias, slabs, part_at):
    proj = slabs[:, :128].reshape(-1, slabs.shape[2])
    mixed = around(*vision_mix(patches, vis_gain[:1], vis_bias[:1], slabs, 6), "mp")
    residual, fed = vision_hidden(
        [side for pair in mixed for side in pair], patches, vis_gain[1:], vis_bias[1:], slabs, 7, 4, 5
    )
    fed = summed_rows(fed)
    own_rows = fed.shape[0]
    own = lax.dynamic_slice_in_dim(residual, part_at * own_rows, own_rows, 0)
    states = (own.astype(jnp.float32) + fed).astype(jnp.bfloat16)
    pooled = jnp.concatenate(ring_halves(pixel_shuffle(states), "mp"), axis=0)
    return dot(pooled, proj).astype(jnp.bfloat16)


def shards(
    text,
    patches,
    segments,
    loss_mask,
    tile_batch,
    tile_offset,
    attn_gain,
    w_query,
    w_kv,
    w_out,
    vis_gain,
    vis_bias,
    v_qkv,
    v_out,
    v_up,
    v_down,
    v_proj,
):
    sections = lax.axis_size("section")
    section_at = lax.axis_index("section")
    part_at = lax.axis_index("mp")
    dp_at = lax.axis_index(DP)
    dp_size = lax.axis_size(DP)
    length = segments.shape[2]

    out_t = v_out.T
    out_t = jnp.concatenate(
        [out_t, *(shifted(out_t, "mp", steps) for steps in (1, -1, 2))], axis=1
    )
    qkv = jnp.concatenate([*v_qkv, jnp.zeros_like(v_qkv[0])], axis=1)
    vision_slab = jnp.concatenate([v_proj, v_up, v_down.T, qkv, out_t], axis=0)
    vision_slab, w_out, loss_mask, text, w_query = lax.optimization_barrier(
        (vision_slab, w_out, loss_mask, text, w_query)
    )
    vision_slabs = lax.all_gather(vision_slab, SECTION_DP)

    parts = lax.axis_size("mp")
    own_out = w_out[0]
    depth = own_out.shape[1]
    rows_each = own_out.shape[0] // (sections * dp_size)
    out_blocks = own_out.reshape(sections, dp_size, rows_each, depth)
    out_blocks = lax.dynamic_index_in_dim(out_blocks, dp_at, 1, keepdims=False)
    out_blocks = exchange(out_blocks, "section")
    text_left = shifted(text[0], "mp", 1)
    text_right = shifted(text[0], "mp", -1)
    near = text.shape[1] // 2
    text_far = [
        shifted(text_left[:near], "mp", 1),
        shifted(text_right[near:], "mp", -1),
    ]
    text_full = jnp.zeros((length, depth), text.dtype)
    pieces = ((text[0], 0), (text_left, 6), (text_right, 2), (text_far[0], 4), (text_far[1], 5))
    for piece, ahead in pieces:
        at = (2 * part_at + ahead) % (2 * parts) * near
        text_full = lax.dynamic_update_slice_in_dim(text_full, piece, at, 0)
    first = out_blocks[0].reshape(rows_each, parts, depth // parts).transpose(1, 0, 2)
    count = jnp.sum(loss_mask).astype(jnp.bfloat16)
    first = exchange(
        jnp.concatenate([first, jnp.broadcast_to(count, first.shape)], axis=1), "mp"
    )
    slab = pack(dp_at, dp_size, w_query, w_kv, attn_gain.reshape(-1, 1), first)
    slab, out_blocks = lax.optimization_barrier((slab, out_blocks))
    slabs = lax.all_gather(slab, SECTION_DP)
    own = out_blocks[1:]
    left = shifted(own, "mp", 1)
    right = shifted(own, "mp", -1)
    far = jnp.concatenate([shifted(left[:1], "mp", 1), shifted(right[1:], "mp", -1)], axis=0)
    out_middle = lax.all_gather(
        jnp.stack([own[:2], left[:2], right[:2], far[:2]]), SECTION_DP
    )
    out_last = lax.all_gather(jnp.stack([own[2:], left[2:], right[2:], far[2:]]), SECTION_DP)

    embedded = encode_tiles(patches, vis_gain, vis_bias, vision_slabs, part_at)

    tiles_here = embedded.shape[0] // POOL
    batch_all = tile_batch[0]
    offset_all = tile_offset[0]
    own_batch = lax.dynamic_slice_in_dim(batch_all, section_at * tiles_here, tiles_here, 0)
    capacity = tiles_here // 2
    block_rows = capacity * POOL
    local_ids = jnp.arange(tiles_here, dtype=jnp.int32)
    local_same = (own_batch[:, None] == own_batch[None, :]) & (
        local_ids[None, :] < local_ids[:, None]
    )
    local_rank = jnp.sum(local_same.astype(jnp.int32), axis=1)
    send_rows = jnp.arange(sections * block_rows, dtype=jnp.int32)
    send_target = (section_at + send_rows // block_rows) % sections
    send_rank = send_rows % block_rows // POOL
    send_match = (own_batch[None, :] == send_target[:, None]) & (
        local_rank[None, :] == send_rank[:, None]
    )
    straight = jnp.arange(parts, dtype=jnp.int32)
    ring = (part_at + jnp.array([0, 3, 1, 2], jnp.int32)) % parts
    each = tiles_here * POOL // parts
    own_rows = (ring[:, None] * each + jnp.arange(each, dtype=jnp.int32)[None, :]).reshape(-1)
    own_tile = jnp.arange(tiles_here, dtype=jnp.int32)[None, :, None] == (own_rows // POOL)
    send_pick = jnp.any(send_match[:, :, None] & own_tile, axis=1) & (
        (own_rows % POOL)[None, :] == (send_rows % POOL)[:, None]
    )
    blocks = dot(send_pick.astype(jnp.bfloat16), embedded).astype(jnp.bfloat16)
    blocks = [blocks[t * block_rows : (t + 1) * block_rows] for t in range(sections)]
    arrived = jnp.concatenate(
        [blocks[0], *(shifted(blocks[t], "section", t) for t in range(1, sections))], axis=0
    )
    arrived_all = ring_halves(arrived, "mp")
    tile_ids = jnp.arange(batch_all.shape[0], dtype=jnp.int32)
    source_ids = tile_ids // tiles_here
    tile_same = (
        (batch_all[:, None] == batch_all[None, :])
        & (source_ids[:, None] == source_ids[None, :])
        & (tile_ids[None, :] < tile_ids[:, None])
    )
    tile_rank = jnp.sum(tile_same.astype(jnp.int32), axis=1)
    slot_rows = jnp.arange(sections * block_rows, dtype=jnp.int32)
    slot_source = (section_at - slot_rows // block_rows) % sections
    slot_rank = slot_rows % block_rows // POOL
    match = (
        (batch_all[None, :] == section_at)
        & (source_ids[None, :] == slot_source[:, None])
        & (tile_rank[None, :] == slot_rank[:, None])
    )
    slot_place = jnp.sum(match.astype(jnp.int32) * offset_all[None, :], axis=1) + slot_rows % POOL
    slot_valid = jnp.any(match, axis=1)
    places = jnp.arange(length, dtype=jnp.int32)
    picker = ((places[:, None] == slot_place[None, :]) & slot_valid[None, :]).astype(jnp.bfloat16)
    covered = jnp.any(
        (batch_all[None, :] == section_at)
        & (places[:, None] >= offset_all[None, :])
        & (places[:, None] < offset_all[None, :] + POOL),
        axis=1,
    )
    columns = depth // parts
    state = jnp.stack(
        [
            jnp.where(
                covered[:, None],
                dot(picker, arrived_all[i]).astype(jnp.bfloat16),
                lax.dynamic_slice_in_dim(text_full, ring[i] * columns, columns, 1),
            )
            for i in range(parts)
        ]
    )

    counts = slabs[:, SLAB_ROWS + 64 :: 16, 512::128]
    totals = jnp.sum(counts.astype(jnp.float32))
    scaling = float(sections * dp_size * length)
    token_weight = loss_mask.astype(jnp.float32) * scaling / totals

    segment_ids = segments[0, 0]
    tables = rope_tables(length)
    shard_rows = text.shape[1]
    width = w_query.shape[2] + 2 * w_kv.shape[3]
    ahead = jnp.sum(jnp.where(straight[:, None] == ring[None, :], straight[None, :], 0), axis=1)
    filler = jnp.zeros((1,), jnp.int32)
    in_ring = jnp.concatenate([straight, filler, ahead])
    in_order = jnp.concatenate([straight, filler, straight])
    for layer in range(sections):
        first, second = attend(
            state,
            ring if layer < 2 else straight,
            slabs,
            layer,
            dp_size,
            width,
            tables,
            segment_ids[:, None],
            segment_ids[None, :],
        )
        if layer == sections - 1:
            both = jnp.concatenate([first, second], axis=1)
            both = both.reshape(parts, shard_rows, -1)
            mine = []
            for steps in (0, 1, -1, 2):
                at = (part_at + steps) % parts
                block = lax.dynamic_index_in_dim(both, at, 0, keepdims=False)
                mine.append(shifted(block, "mp", steps) if steps else block)
            state = lax.dynamic_slice_in_dim(state, part_at * shard_rows, shard_rows, 0)
            state = project_whole(mine, in_order, out_last, 0, state)
        else:
            mixes = [side for both in around(first, second, "mp") for side in both]
            if layer == 0:
                own_columns, token_weight = lax.optimization_barrier(
                    (project_columns(mixes, ring, slabs, state), token_weight)
                )
                state = jnp.stack(ring_halves(own_columns, "mp"))
            else:
                order = in_ring if layer == 1 else in_order
                state = project_whole(mixes, order, out_middle, layer - 1, state)

    return (state[None], token_weight)


def solution(mesh):
    split = Mesh(
        mesh.devices.reshape(mesh.shape["section"], 4, 2, mesh.shape["mp"]),
        ("section", "dp_0", "dp_1", "mp"),
    )
    return jax.shard_map(
        shards,
        mesh=split,
        in_specs=(
            P("section", DP_MP, None),
            P(SECTION_DP, None),
            P("section", DP, None),
            P("section", DP_MP),
            P(DP, None),
            P(DP, None),
            P("section", None),
            P("section", None, "mp"),
            P("section", None, None, "mp"),
            P("section", "mp", None),
            P(),
            P(),
            P(None, SECTION_DP, "mp"),
            P("mp", SECTION_DP),
            P(SECTION_DP, "mp"),
            P("mp", SECTION_DP),
            P(SECTION_DP, "mp"),
        ),
        out_specs=(P("section", DP_MP, None), P("section", DP_MP)),
        check_vma=False,
    )
```

```python
import jax
import jax.numpy as jnp
from jax import lax
from jax.experimental import pallas as pl
from jax.experimental.pallas import tpu as pltpu
from jax.sharding import Mesh
from jax.sharding import PartitionSpec as P


HD = 128
VHD = 64
GRID = 16
PATCH = 256
POOL = 64
SECTION_DP = ("section", "dp_0", "dp_1")
DP = ("dp_0", "dp_1")
DP_MP = ("dp_0", "dp_1", "mp")


EPS = 1e-05
ROPE_BASE = 500000.0
BLOCKED = -1e30
ROW_BLOCK = 256
SLAB_ROWS = 512
MIB = 1024 * 1024


def dot(left, right):
    return jnp.dot(left, right, preferred_element_type=jnp.float32)


def exchange(blocks, axis):
    return lax.all_to_all(blocks, axis, split_axis=0, concat_axis=0, tiled=True)


def shifted(value, axis, steps):
    count = lax.axis_size(axis)
    pairs = [(source, (source + steps) % count) for source in range(count)]
    return lax.ppermute(value, axis, pairs)


def around(first, second, axis):
    left_first = shifted(first, axis, 1)
    right_second = shifted(second, axis, -1)
    left_second = shifted(second, axis, 1)
    right_first = shifted(first, axis, -1)
    far_first = shifted(left_first, axis, 1)
    far_second = shifted(right_second, axis, -1)
    return (
        (first, second),
        (left_first, left_second),
        (right_first, right_second),
        (far_first, far_second),
    )


def ring_halves(array, axis):
    half = array.shape[0] // 2
    left, right = shifted(array, axis, 1), shifted(array, axis, -1)
    far = (shifted(left[:half], axis, 1), shifted(right[half:], axis, -1))
    return array, left, right, jnp.concatenate(far, axis=0)


def layer_norm(values, gain, bias):
    wide = values.astype(jnp.float32)
    center = wide - jnp.mean(wide, axis=-1, keepdims=True)
    spread = jnp.mean(center * center, axis=-1, keepdims=True)
    return (center * lax.rsqrt(spread + EPS) * gain + bias).astype(jnp.bfloat16)


def rope_tables(length):
    half = HD // 2
    freqs = ROPE_BASE ** (-2.0 * jnp.arange(half, dtype=jnp.float32) / HD)
    angles = jnp.arange(length, dtype=jnp.float32)[:, None] * freqs[None, :]
    cosine, sine = jnp.cos(angles), jnp.sin(angles)
    return jnp.concatenate([cosine, cosine], axis=1), jnp.concatenate([-sine, sine], axis=1)


def attention_kernel(state_ref, w_ref, cos_ref, sin_ref, seg_col_ref, seg_row_ref, *rest, depth):
    out_refs, (acc_ref, power_ref) = rest[:2], rest[2:]
    step = pl.program_id(0)
    block = state_ref[...]
    wide = block.astype(jnp.float32)
    power = jnp.sum(wide * wide, axis=1, keepdims=True)
    part = dot(block, w_ref[...].reshape(block.shape[1], w_ref.shape[2]))

    @pl.when(step == 0)
    def _():
        acc_ref[...] = part
        power_ref[...] = power

    @pl.when(step > 0)
    def _():
        acc_ref[...] += part
        power_ref[...] += power

    @pl.when(step == pl.num_programs(0) - 1)
    def _():
        heads = acc_ref.shape[1] // HD - 2
        length = acc_ref.shape[0]
        scale = lax.rsqrt(power_ref[...] * (1.0 / depth) + EPS)
        cosine, sine = cos_ref[...], sin_ref[...]

        def column(index):
            return acc_ref[:, index * HD : (index + 1) * HD] * scale

        def rotated(index):
            values = column(index)
            return (values * cosine + pltpu.roll(values, HD // 2, 1) * sine).astype(jnp.bfloat16)

        keyed = rotated(heads)
        valued = column(heads + 1).astype(jnp.bfloat16)
        queries = [rotated(head) for head in range(heads)]
        for begin in range(0, length, ROW_BLOCK):
            end = begin + ROW_BLOCK
            rows = lax.broadcasted_iota(jnp.int32, (ROW_BLOCK, end), 0) + begin
            cols = lax.broadcasted_iota(jnp.int32, (ROW_BLOCK, end), 1)
            allowed = (seg_col_ref[begin:end, :] == seg_row_ref[:, :end]) & (cols <= rows)
            for head in range(heads):
                scores = lax.dot_general(
                    queries[head][begin:end],
                    keyed[:end],
                    (((1,), (1,)), ((), ())),
                    preferred_element_type=jnp.float32,
                ) * HD ** (-0.5)
                scores = jnp.where(allowed, scores, BLOCKED)
                top = jnp.max(scores, axis=1, keepdims=True)
                weights = jnp.exp(scores - top)
                total = jnp.sum(weights, axis=1, keepdims=True)
                mix = dot(weights.astype(jnp.bfloat16), valued[:end]) / total
                side = head * 2 // heads
                at = (head - side * heads // 2) * HD
                out_refs[side][begin:end, at : at + HD] = mix.astype(jnp.bfloat16)


def whole(shape):
    return pl.BlockSpec(shape, lambda *_: (0,) * len(shape))


def params(mib):
    return pltpu.CompilerParams(
        dimension_semantics=("arbitrary",), vmem_limit_bytes=mib * MIB
    )


def state_spec(state, width, index):
    if state.ndim == 2:
        return pl.BlockSpec((state.shape[0], width), lambda n, *s: (0, index(n, *s)))
    per = state.shape[2] // width
    return pl.BlockSpec(
        (None, state.shape[1], width),
        lambda n, *s: (index(n, *s) // per, 0, index(n, *s) % per),
    )


def attend(state, order, slabs, layer, chunks, width, tables, seg_col, seg_row):
    length = state.shape[-2]
    depth = chunks * SLAB_ROWS
    steps = chunks // 2
    rows = depth // chunks
    cosine, sine = tables
    heads = width // HD - 2
    half = jax.ShapeDtypeStruct((length, heads * HD // 2), jnp.bfloat16)
    return pl.pallas_call(
        lambda order_ref, *refs: attention_kernel(*refs, depth=depth),
        grid_spec=pltpu.PrefetchScalarGridSpec(
            num_scalar_prefetch=1,
            grid=(steps,),
            in_specs=[
                state_spec(state, 2 * rows, lambda k, s: k),
                pl.BlockSpec((2, rows, width), lambda k, s: (layer * steps + s[k], 0, 0)),
                whole(cosine.shape),
                whole(sine.shape),
                whole(seg_col.shape),
                whole(seg_row.shape),
            ],
            out_specs=[whole(half.shape), whole(half.shape)],
            scratch_shapes=[
                pltpu.VMEM((length, width), jnp.float32),
                pltpu.VMEM((length, 1), jnp.float32),
            ],
        ),
        out_shape=[half, half],
        compiler_params=params(50),
        cost_estimate=pl.CostEstimate(
            flops=2 * length * depth * width,
            bytes_accessed=2 * depth * (length + width),
            transcendentals=heads * length * length,
        ),
        name="attend",
    )(order, state, slabs, cosine, sine, seg_col, seg_row)


def out_kernel(order_ref, *refs, per_block):
    blocks = (len(refs) - 3) // (per_block + 1)
    mixes, weights = refs[: blocks * per_block], refs[blocks * per_block : -3]
    state_ref, out_ref, joined_ref = refs[-3:]

    @pl.when(pl.program_id(0) == 0)
    def _():
        side = joined_ref.shape[2] // per_block
        for at, mix_ref in enumerate(mixes):
            begin = at % per_block * side
            joined_ref[at // per_block, :, begin : begin + side] = mix_ref[...]

    total = state_ref[...].astype(jnp.float32)
    for at, weight_ref in enumerate(weights):
        size = (joined_ref.shape[2], weight_ref.shape[-1])
        total = total + dot(joined_ref[at], weight_ref[...].reshape(size))
    out_ref[...] = total.astype(jnp.bfloat16)


def project_out(mixes, order, weights, weight_block, weight_index, state, steps, state_index):
    rows = state.shape[-2]
    width = weight_block[-1]
    per_block = weights.shape[0] * weight_block[-2]
    blocks = 4
    weight_spec = lambda j: pl.BlockSpec(weight_block, lambda n, s: weight_index(n, s[j]))
    return pl.pallas_call(
        lambda *refs: out_kernel(*refs, per_block=len(mixes) // blocks),
        grid_spec=pltpu.PrefetchScalarGridSpec(
            num_scalar_prefetch=1,
            grid=(steps,),
            in_specs=[whole(m.shape) for m in mixes]
            + [weight_spec(j) for j in range(blocks)]
            + [state_spec(state, width, state_index)],
            out_specs=pl.BlockSpec((rows, width), lambda n, s: (0, n)),
            scratch_shapes=[pltpu.VMEM((blocks, rows, per_block), jnp.bfloat16)],
        ),
        out_shape=jax.ShapeDtypeStruct((rows, steps * width), jnp.bfloat16),
        compiler_params=params(50),
        cost_estimate=pl.CostEstimate(
            flops=2 * rows * blocks * per_block * steps * width,
            bytes_accessed=2 * steps * width * (blocks * per_block + 2 * rows),
            transcendentals=0,
        ),
        name="project_out",
    )(order, *mixes, *([weights] * blocks), state)


def project_whole(mixes, order, pair, layer, state):
    spread, lines, depth = pair.shape[0], pair.shape[3], pair.shape[4]
    width = 1024
    return project_out(
        mixes,
        order,
        pair,
        (spread, 1, 1, lines, width),
        lambda n, block: (0, block, layer, 0, n),
        state,
        depth // width,
        lambda n, s: s[5 + n],
    )


def project_columns(mixes, order, slabs, state):
    lines, width = 16, 256
    row_at = SLAB_ROWS // lines
    steps = 4
    return project_out(
        mixes,
        order,
        slabs,
        (slabs.shape[0], lines, width),
        lambda n, block: (
            0,
            row_at + block + n // 3 * (4 + block % 2 - block),
            n % 3 + n // 3 * (block // 2),
        ),
        state,
        steps,
        lambda n, s: n,
    )


def pack_kernel(at_ref, q_ref, kv_ref, gain_ref, first_ref, out_ref):
    gain = gain_ref[...]
    rows = q_ref.shape[1]
    scaled = lambda block: (block.astype(jnp.float32) * gain).astype(jnp.bfloat16)
    out_ref[:rows, :512] = scaled(q_ref[0])
    out_ref[:rows, 512:640] = scaled(kv_ref[0, 0])
    out_ref[:rows, 640:768] = scaled(kv_ref[0, 1])
    for part in range(4):
        at = rows + part * 16
        out_ref[at : at + 16] = first_ref[part, :16, :768]
        at, begin = rows + 64 + part % 2 * 16, part // 2 * 256
        out_ref[at : at + 16, begin : begin + 256] = first_ref[part, :16, 768:]
        begin = 512 + part // 2 * 128
        out_ref[at : at + 16, begin : begin + 128] = first_ref[part, 16:, :128]


def pack(dp_at, dp_size, w_query, w_kv, gain, first):
    rows = w_query.shape[1] // dp_size
    shape = (rows + 96, 768)
    return pl.pallas_call(
        pack_kernel,
        grid_spec=pltpu.PrefetchScalarGridSpec(
            num_scalar_prefetch=1,
            grid=(1,),
            in_specs=[
                pl.BlockSpec((1, rows, w_query.shape[2]), lambda n, s: (0, s[0], 0)),
                pl.BlockSpec((1, 2, rows, w_kv.shape[3]), lambda n, s: (0, 0, s[0], 0)),
                pl.BlockSpec((rows, 1), lambda n, s: (s[0], 0)),
                whole(first.shape),
            ],
            out_specs=whole(shape),
        ),
        out_shape=jax.ShapeDtypeStruct(shape, jnp.bfloat16),
        compiler_params=params(56),
        name="pack",
    )(dp_at[None], w_query, w_kv, gain, first)


def vision_mix_kernel(patches_ref, gain_ref, bias_ref, qkv_ref, *out_refs):
    normed = layer_norm(patches_ref[...], gain_ref[...], bias_ref[...])
    weights = qkv_ref[...].reshape(normed.shape[1], qkv_ref.shape[2])
    projected = dot(normed, weights).astype(jnp.bfloat16)
    width = projected.shape[1] // 3
    pair = 2 * VHD
    lower = lax.broadcasted_iota(jnp.int32, (PATCH, pair), 1) < VHD
    for begin in range(0, projected.shape[0], PATCH):
        for at in range(0, width, pair):
            query, keyed, valued = (
                projected[begin : begin + PATCH, i * width + at : i * width + at + pair]
                for i in range(3)
            )
            mixes = []
            for mine in (lower, ~lower):
                scores = lax.dot_general(
                    jnp.where(mine, query, jnp.zeros_like(query)),
                    keyed,
                    (((1,), (1,)), ((), ())),
                    preferred_element_type=jnp.float32,
                ) * VHD ** (-0.5)
                top = jnp.max(scores, axis=1, keepdims=True)
                grown = jnp.exp(scores - top)
                total = jnp.sum(grown, axis=1, keepdims=True)
                mixes.append(dot(grown.astype(jnp.bfloat16), valued) / total)
            mixed = jnp.where(lower, mixes[0], mixes[1])
            out_refs[begin // PATCH][:, at : at + pair] = mixed.astype(jnp.bfloat16)


def vision_mix(patches, gain, bias, slabs, at):
    width = 768
    return pl.pallas_call(
        vision_mix_kernel,
        grid=(1,),
        in_specs=[
            whole(patches.shape),
            whole(gain.shape),
            whole(bias.shape),
            pl.BlockSpec((slabs.shape[0], 32, width), lambda n: (0, at, 0)),
        ],
        out_specs=[whole((PATCH, width // 3))] * 2,
        out_shape=[jax.ShapeDtypeStruct((PATCH, width // 3), jnp.bfloat16)] * 2,
        compiler_params=params(40),
        name="vision_mix",
    )(patches, gain, bias, slabs)


def vision_hidden_kernel(*refs):
    mixed_refs, out_t_refs, rest = refs[:8], refs[8:12], refs[12:]
    patches_ref, gain_ref, bias_ref, up_ref, down_ref, rest_ref, fed_ref = rest
    contract_last = (((1,), (1,)), ((), ()))
    total = patches_ref[...].astype(jnp.float32)
    for part in range(4):
        both = [mixed_refs[2 * part + side][...] for side in range(2)]
        total = total + lax.dot_general(
            jnp.concatenate(both, axis=0),
            out_t_refs[part][...],
            contract_last,
            preferred_element_type=jnp.float32,
        )
    residual = total.astype(jnp.bfloat16)
    rest_ref[...] = residual
    normed = layer_norm(residual, gain_ref[...], bias_ref[...])
    width = normed.shape[1]
    inner = dot(normed, up_ref[...].reshape(width, width))
    inner = (0.5 * inner * (1.0 + lax.erf(inner * 2.0**-0.5))).astype(jnp.bfloat16)
    fed = lax.dot_general(
        inner,
        down_ref[...].reshape(width, width),
        contract_last,
        preferred_element_type=jnp.float32,
    )
    fed_ref[...] = fed.astype(jnp.bfloat16)


def vision_hidden(gathered, out_t, patches, gain, bias, slabs, up_at, down_at):
    width = patches.shape[1]
    block = lambda at: pl.BlockSpec((slabs.shape[0], 32, width), lambda n: (0, at, 0))
    both = jax.ShapeDtypeStruct(patches.shape, jnp.bfloat16)
    return pl.pallas_call(
        vision_hidden_kernel,
        grid=(1,),
        in_specs=[
            *[whole(part.shape) for part in gathered],
            *[whole(part.shape) for part in out_t],
            whole(patches.shape),
            whole(gain.shape),
            whole(bias.shape),
            block(up_at),
            block(down_at),
        ],
        out_specs=[whole(patches.shape), whole(patches.shape)],
        out_shape=[both, both],
        compiler_params=params(40),
        name="vision_hidden",
    )(*gathered, *out_t, patches, gain, bias, slabs, slabs)


def pixel_shuffle(states):
    rows, width = states.shape
    side_half = GRID // 2
    arranged = states.reshape(rows // (2 * GRID), 2, side_half, 2, width)
    return arranged.transpose(0, 2, 1, 3, 4).reshape(rows // 4, 4 * width)


def summed_rows(partial):
    blocks = partial.reshape(lax.axis_size("mp"), -1, partial.shape[1])
    return jnp.sum(exchange(blocks, "mp").astype(jnp.float32), axis=0)


def encode_tiles(patches, vis_gain, vis_bias, slabs, part_at):
    proj = slabs[:, :128].reshape(-1, slabs.shape[2])
    out_t = ring_halves(slabs[:, 192:224, 768:].reshape(-1, 256), "mp")
    mixed = around(*vision_mix(patches, vis_gain[:1], vis_bias[:1], slabs, 6), "mp")
    residual, fed = vision_hidden(
        [side for pair in mixed for side in pair],
        out_t,
        patches,
        vis_gain[1:],
        vis_bias[1:],
        slabs,
        4,
        5,
    )
    fed = summed_rows(fed)
    own_rows = fed.shape[0]
    own = lax.dynamic_slice_in_dim(residual, part_at * own_rows, own_rows, 0)
    states = (own.astype(jnp.float32) + fed).astype(jnp.bfloat16)
    pooled = jnp.concatenate(ring_halves(pixel_shuffle(states), "mp"), axis=0)
    return dot(pooled, proj).astype(jnp.bfloat16)


def shards(
    text,
    patches,
    segments,
    loss_mask,
    tile_batch,
    tile_offset,
    attn_gain,
    w_query,
    w_kv,
    w_out,
    vis_gain,
    vis_bias,
    v_qkv,
    v_out,
    v_up,
    v_down,
    v_proj,
):
    sections = lax.axis_size("section")
    section_at = lax.axis_index("section")
    part_at = lax.axis_index("mp")
    dp_at = lax.axis_index(DP)
    dp_size = lax.axis_size(DP)
    length = segments.shape[2]

    qkv = jnp.concatenate([*v_qkv, v_out.T], axis=1)
    vision_slab = jnp.concatenate([v_proj, v_up, v_down.T, qkv], axis=0)
    vision_slab, w_out, loss_mask, text, w_query = lax.optimization_barrier(
        (vision_slab, w_out, loss_mask, text, w_query)
    )
    vision_slabs = lax.all_gather(vision_slab, SECTION_DP)

    parts = lax.axis_size("mp")
    own_out = w_out[0]
    depth = own_out.shape[1]
    rows_each = own_out.shape[0] // (sections * dp_size)
    out_blocks = own_out.reshape(sections, dp_size, rows_each, depth)
    out_blocks = lax.dynamic_index_in_dim(out_blocks, dp_at, 1, keepdims=False)
    out_blocks = exchange(out_blocks, "section")
    text_left = shifted(text[0], "mp", 1)
    text_right = shifted(text[0], "mp", -1)
    near = text.shape[1] // 2
    text_far = [
        shifted(text_left[:near], "mp", 1),
        shifted(text_right[near:], "mp", -1),
    ]
    text_full = jnp.zeros((length, depth), text.dtype)
    pieces = ((text[0], 0), (text_left, 6), (text_right, 2), (text_far[0], 4), (text_far[1], 5))
    for piece, ahead in pieces:
        at = (2 * part_at + ahead) % (2 * parts) * near
        text_full = lax.dynamic_update_slice_in_dim(text_full, piece, at, 0)
    first = out_blocks[0].reshape(rows_each, parts, depth // parts).transpose(1, 0, 2)
    count = jnp.sum(loss_mask).astype(jnp.bfloat16)
    first = exchange(
        jnp.concatenate([first, jnp.broadcast_to(count, first.shape)], axis=1), "mp"
    )
    slab = pack(dp_at, dp_size, w_query, w_kv, attn_gain.reshape(-1, 1), first)
    slab, out_blocks = lax.optimization_barrier((slab, out_blocks))
    slabs = lax.all_gather(slab, SECTION_DP)
    own = out_blocks[1:]
    left = shifted(own, "mp", 1)
    right = shifted(own, "mp", -1)
    far = jnp.concatenate([shifted(left[:1], "mp", 1), shifted(right[1:], "mp", -1)], axis=0)
    out_middle = lax.all_gather(
        jnp.stack([own[:2], left[:2], right[:2], far[:2]]), SECTION_DP
    )
    out_last = lax.all_gather(jnp.stack([own[2:], left[2:], right[2:], far[2:]]), SECTION_DP)

    embedded = encode_tiles(patches, vis_gain, vis_bias, vision_slabs, part_at)

    tiles_here = embedded.shape[0] // POOL
    batch_all = tile_batch[0]
    offset_all = tile_offset[0]
    own_batch = lax.dynamic_slice_in_dim(batch_all, section_at * tiles_here, tiles_here, 0)
    capacity = tiles_here // 2
    block_rows = capacity * POOL
    local_ids = jnp.arange(tiles_here, dtype=jnp.int32)
    local_same = (own_batch[:, None] == own_batch[None, :]) & (
        local_ids[None, :] < local_ids[:, None]
    )
    local_rank = jnp.sum(local_same.astype(jnp.int32), axis=1)
    send_rows = jnp.arange(sections * block_rows, dtype=jnp.int32)
    send_target = (section_at + send_rows // block_rows) % sections
    send_rank = send_rows % block_rows // POOL
    send_match = (own_batch[None, :] == send_target[:, None]) & (
        local_rank[None, :] == send_rank[:, None]
    )
    straight = jnp.arange(parts, dtype=jnp.int32)
    ring = (part_at + jnp.array([0, 3, 1, 2], jnp.int32)) % parts
    each = tiles_here * POOL // parts
    own_rows = (ring[:, None] * each + jnp.arange(each, dtype=jnp.int32)[None, :]).reshape(-1)
    own_tile = jnp.arange(tiles_here, dtype=jnp.int32)[None, :, None] == (own_rows // POOL)
    send_pick = jnp.any(send_match[:, :, None] & own_tile, axis=1) & (
        (own_rows % POOL)[None, :] == (send_rows % POOL)[:, None]
    )
    blocks = dot(send_pick.astype(jnp.bfloat16), embedded).astype(jnp.bfloat16)
    blocks = [blocks[t * block_rows : (t + 1) * block_rows] for t in range(sections)]
    arrived = jnp.concatenate(
        [blocks[0], *(shifted(blocks[t], "section", t) for t in range(1, sections))], axis=0
    )
    arrived_all = ring_halves(arrived, "mp")
    tile_ids = jnp.arange(batch_all.shape[0], dtype=jnp.int32)
    source_ids = tile_ids // tiles_here
    tile_same = (
        (batch_all[:, None] == batch_all[None, :])
        & (source_ids[:, None] == source_ids[None, :])
        & (tile_ids[None, :] < tile_ids[:, None])
    )
    tile_rank = jnp.sum(tile_same.astype(jnp.int32), axis=1)
    slot_rows = jnp.arange(sections * block_rows, dtype=jnp.int32)
    slot_source = (section_at - slot_rows // block_rows) % sections
    slot_rank = slot_rows % block_rows // POOL
    match = (
        (batch_all[None, :] == section_at)
        & (source_ids[None, :] == slot_source[:, None])
        & (tile_rank[None, :] == slot_rank[:, None])
    )
    slot_place = jnp.sum(match.astype(jnp.int32) * offset_all[None, :], axis=1) + slot_rows % POOL
    slot_valid = jnp.any(match, axis=1)
    places = jnp.arange(length, dtype=jnp.int32)
    picker = ((places[:, None] == slot_place[None, :]) & slot_valid[None, :]).astype(jnp.bfloat16)
    covered = jnp.any(
        (batch_all[None, :] == section_at)
        & (places[:, None] >= offset_all[None, :])
        & (places[:, None] < offset_all[None, :] + POOL),
        axis=1,
    )
    columns = depth // parts
    state = jnp.stack(
        [
            jnp.where(
                covered[:, None],
                dot(picker, arrived_all[i]).astype(jnp.bfloat16),
                lax.dynamic_slice_in_dim(text_full, ring[i] * columns, columns, 1),
            )
            for i in range(parts)
        ]
    )

    counts = slabs[:, SLAB_ROWS + 64 :: 16, 512::128]
    totals = jnp.sum(counts.astype(jnp.float32))
    scaling = float(sections * dp_size * length)
    token_weight = loss_mask.astype(jnp.float32) * scaling / totals

    segment_ids = segments[0, 0]
    tables = rope_tables(length)
    shard_rows = text.shape[1]
    width = w_query.shape[2] + 2 * w_kv.shape[3]
    ahead = jnp.sum(jnp.where(straight[:, None] == ring[None, :], straight[None, :], 0), axis=1)
    filler = jnp.zeros((1,), jnp.int32)
    in_ring = jnp.concatenate([straight, filler, ahead])
    in_order = jnp.concatenate([straight, filler, straight])
    for layer in range(sections):
        first, second = attend(
            state,
            ring if layer < 2 else straight,
            slabs,
            layer,
            dp_size,
            width,
            tables,
            segment_ids[:, None],
            segment_ids[None, :],
        )
        if layer == sections - 1:
            both = jnp.concatenate([first, second], axis=1)
            both = both.reshape(parts, shard_rows, -1)
            mine = []
            for steps in (0, 1, -1, 2):
                at = (part_at + steps) % parts
                block = lax.dynamic_index_in_dim(both, at, 0, keepdims=False)
                mine.append(shifted(block, "mp", steps) if steps else block)
            state = lax.dynamic_slice_in_dim(state, part_at * shard_rows, shard_rows, 0)
            state = project_whole(mine, in_order, out_last, 0, state)
        else:
            mixes = [side for both in around(first, second, "mp") for side in both]
            if layer == 0:
                own_columns, token_weight = lax.optimization_barrier(
                    (project_columns(mixes, ring, slabs, state), token_weight)
                )
                state = jnp.stack(ring_halves(own_columns, "mp"))
            else:
                order = in_ring if layer == 1 else in_order
                state = project_whole(mixes, order, out_middle, layer - 1, state)

    return (state[None], token_weight)


def solution(mesh):
    split = Mesh(
        mesh.devices.reshape(mesh.shape["section"], 4, 2, mesh.shape["mp"]),
        ("section", "dp_0", "dp_1", "mp"),
    )
    return jax.shard_map(
        shards,
        mesh=split,
        in_specs=(
            P("section", DP_MP, None),
            P(SECTION_DP, None),
            P("section", DP, None),
            P("section", DP_MP),
            P(DP, None),
            P(DP, None),
            P("section", None),
            P("section", None, "mp"),
            P("section", None, None, "mp"),
            P("section", "mp", None),
            P(),
            P(),
            P(None, SECTION_DP, "mp"),
            P("mp", SECTION_DP),
            P(SECTION_DP, "mp"),
            P("mp", SECTION_DP),
            P(SECTION_DP, "mp"),
        ),
        out_specs=(P("section", DP_MP, None), P("section", DP_MP)),
        check_vma=False,
    )
```
